128 devices in a mesh: rows: 16 (over x, z), cols: 8 (over y, core).
Axes of the slice: x: 4, y: 4, z: 4, core: 2. Of those that a mesh axis runs over, the one named last changes fastest.
Arguments:
- bag_index: int32 [2048, 128], P(('rows', 'cols')), may hold values from 0 to 1048575, as said below
- bag_length: int32 [2048, 4], P(('rows', 'cols')), may hold values from 1 to 32
- emb_tables: float32 [4, 1048576, 128], P(None, ('rows', 'cols')), may hold values from -0.6 to 0.6
- dense_feats: float32 [2048, 128], P(('rows', 'cols')), may hold values from -6 to 6
- w_dense: float32 [128, 1024], replicated, may hold values from -0.5 to 0.5
- w_pair: float32 [10, 1024], replicated, may hold values from -0.5 to 0.5
- top_bias: float32 [1024], replicated, may hold values from -3 to 3
Outputs:
- pooled: float32 [2048, 4, 128], P(('rows', 'cols'))
- top_hidden: float32 [2048, 1024], P(('rows', 'cols'))
The draws below stay inside these ranges and needn't reach their ends.
Inputs may be any that keep to these rules, and one draw needn't show every extreme that they name: `bag_length`: slots at or past a bag's length are ignored, whatever they hold. `bag_index`: device d holds rows d * 8192 to (d + 1) * 8192 - 1 of every table; among the 2048 slots (live or not) of the samples of one device, at most 32 hold rows of any one device, and in every draw some device's rows receive exactly 32 slots from every device.
All inputs are finite; a program needn't handle non-finite values.
Results may differ from the reference program's by a relative error of at most 0.0001.
Values sent between devices are 32-bit elements; how exact they have to be, the bound alone decides.
A program may use at most 128 MiB of HBM per device.

```python
import jax
import jax.numpy as jnp
from jax import lax

E = 128
ROWS_DEV = 8192
NT = 4
L = 32
H = 1024
SAMP_DEV = 16
B = 2048
VOCAB = 1048576
PAIRS = 10


def draw_bag_index(key, part):
    ndevices = B // SAMP_DEV
    slots = SAMP_DEV * NT * L
    capacity = 2 * slots // ndevices
    total = ndevices * capacity
    token_owner = jnp.arange(total, dtype=jnp.int32) // capacity
    key_weight, key_common, key_blocks = jax.random.split(key, 3)
    weight = jax.random.randint(key_weight, (ndevices,), 0, 4, dtype=jnp.int32) * 512
    common_hot = jax.random.randint(key_common, (), 0, ndevices, dtype=jnp.int32)

    def one_block(block_key):
        key_own, key_score, key_order, key_first, key_second = jax.random.split(block_key, 5)
        own_hot = jax.random.randint(key_own, (), 0, ndevices, dtype=jnp.int32)
        forced = jnp.where((token_owner == common_hot) | (token_owner == own_hot), 4096, 0).astype(jnp.int32)
        score = jax.random.randint(key_score, (total,), 0, 1024, dtype=jnp.int32) + weight[token_owner] + forced
        score = score * total + jnp.arange(total, dtype=jnp.int32)
        unused, chosen = lax.top_k(score, slots)
        order = jax.random.permutation(key_order, slots)
        owners = token_owner[chosen[order]]
        first_draw = jax.random.randint(key_first, (slots,), 0, ROWS_DEV, dtype=jnp.int32)
        second_draw = jax.random.randint(key_second, (slots,), 1, ROWS_DEV + 1, dtype=jnp.int32)
        local = first_draw * second_draw // ROWS_DEV
        return (owners * ROWS_DEV + local).reshape(SAMP_DEV, NT * L)
    block_keys = jax.random.split(key_blocks, ndevices)
    return jax.vmap(one_block)(block_keys).reshape(B, NT * L).astype(jnp.int32)


def touch_ends(drawn, own_key, least, largest):
    dims = drawn.shape
    spot = [jax.random.randint(jax.random.fold_in(own_key, axis), (), 0, dims[axis]) for axis in range(len(dims))]
    drawn = drawn.at[tuple(spot)].set(least)
    longest = dims.index(max(dims))
    spot[longest] = (spot[longest] + 1) % dims[longest]
    return drawn.at[tuple(spot)].set(largest)


def block_scale(own_key, extent, cuts, smallest, largest):
    factor_of = 1.0
    for axis_at, parts in cuts:
        draws = jax.random.uniform(jax.random.fold_in(jax.random.fold_in(own_key, 6), axis_at), (parts,), jnp.float32, smallest / len(cuts), largest / len(cuts))
        factor_of = factor_of * jnp.repeat(jnp.exp(draws), extent[axis_at] // parts).reshape((-1,) + (1,) * (len(extent) - 1 - axis_at))
    return factor_of


def normal_values(stream_key, shape, spread, bound, cuts=(), held_as=jnp.bfloat16):
    drawn = spread * jax.random.normal(stream_key, shape, jnp.float32)
    if cuts:
        drawn = drawn * block_scale(stream_key, shape, cuts, -0.22, 0.18)
    return jnp.clip(drawn, -bound, bound).astype(held_as)


def setup_inputs(seed: int = 0) -> dict:
    seeds = jax.random.split(jax.random.key(seed), 8)
    return {
        "bag_index": draw_bag_index(jax.random.fold_in(seeds[7], 71), 0),
        "bag_length": touch_ends(jax.random.randint(seeds[1], (B, NT), 1, L + 1), jax.random.fold_in(seeds[1], 1), 1, L).astype(jnp.int32),
        "emb_tables": normal_values(seeds[2], (NT, VOCAB, E), 0.1, 0.6, ((1, 128),), jnp.float32),
        "dense_feats": normal_values(seeds[3], (B, E), 1.0, 6.0, ((0, 128),), jnp.float32),
        "w_dense": normal_values(seeds[4], (E, H), (E + PAIRS) ** -0.5, 0.5, (), jnp.float32),
        "w_pair": normal_values(seeds[5], (PAIRS, H), (E + PAIRS) ** -0.5, 0.5, (), jnp.float32),
        "top_bias": normal_values(seeds[6], (H,), 0.5, 3.0, (), jnp.float32),
    }


def interact(dense_feats, pooled, w_dense, w_pair, top_bias):
    feats = [dense_feats] + [pooled[:, t, :] for t in range(NT)]
    pair_list = []
    for first in range(NT + 1):
        for second in range(first + 1, NT + 1):
            pair_list.append(jnp.sum(feats[first] * feats[second], axis=-1))
    pair_dots = jnp.stack(pair_list, axis=1)
    hidden = jnp.dot(dense_feats, w_dense, precision=lax.Precision.HIGHEST, preferred_element_type=jnp.float32)
    hidden = hidden + jnp.dot(pair_dots, w_pair, precision=lax.Precision.HIGHEST, preferred_element_type=jnp.float32)
    return jnp.maximum(hidden + top_bias, 0.0)


def reference(bag_index, bag_length, emb_tables, dense_feats, w_dense, w_pair, top_bias):
    position = jnp.arange(L, dtype=jnp.int32)
    pieces = []
    for table in range(NT):
        ids = bag_index[:, table * L:(table + 1) * L]
        live = position[None, :] < bag_length[:, table:table + 1]
        picked = jnp.take(emb_tables[table], ids, axis=0)
        pieces.append(jnp.sum(jnp.where(live[:, :, None], picked, 0.0), axis=1))
    pooled = jnp.stack(pieces, axis=1)
    return pooled, interact(dense_feats, pooled, w_dense, w_pair, top_bias)
```

```python
import functools

import jax
import jax.numpy as jnp
from jax import lax
from jax.experimental import pallas as pl
from jax.experimental.pallas import tpu as pltpu
from jax.sharding import PartitionSpec as P

MESH = pl.DeviceIdType.MESH
F32 = jnp.float32
BF16 = jnp.bfloat16
I32 = jnp.int32
SIDE = 4
CHIPS = SIDE**3
CHUNKS = 8
LAG = 5
AHEAD = 3
CUT = (0, 24, 48, 64)


def kernel(
    dims,
    index_hbm,
    length_hbm,
    table_hbm,
    dense_hbm,
    wd_hbm,
    wp_hbm,
    bias_hbm,
    pooled_ref,
    hidden_ref,
    index_ref,
    length_ref,
    dense_ref,
    wp_ref,
    bias_ref,
    table,
    wd,
    hidden,
    outbox,
    inbox,
    matebox,
    ids_own,
    ids_mate,
    mate_out,
    rows_all,
    a_out,
    a_in,
    b_out,
    b_in,
    input_sem,
    table_sem,
    box_send,
    box_recv,
    fwd_send,
    fwd_recv,
    own_sem,
    mate_sem,
    rows_send,
    rows_recv,
    a_send,
    x_recv,
    y_recv,
    z_recv,
    b_send,
    b_recv,
):
    local_rows, nt, slots_bag, cap = dims
    n = 2 * CHIPS
    samples, lanes = index_ref.shape
    bags = samples * nt
    total_rows = nt * local_rows
    r = lax.axis_index("rows")
    c = lax.axis_index("cols")
    x, z, y, k = r // SIDE, r % SIDE, c // 2, c % 2

    def step_by(at, d):
        return (at + d) % SIDE

    def device(xx, yy, zz, kk):
        return {"rows": xx * SIDE + zz, "cols": yy * 2 + kk}

    offsets = [
        (dx, dy, dz) for dz in range(SIDE) for dy in range(SIDE) for dx in range(SIDE) if dx or dy or dz
    ]
    offsets.sort(key=lambda o: -sum(min(d, SIDE - d) for d in o))

    inputs = [
        pltpu.make_async_copy(source, target, input_sem.at[i])
        for i, (source, target) in enumerate(
            (
                (index_hbm, index_ref),
                (length_hbm, length_ref),
                (wd_hbm, wd),
                (dense_hbm, dense_ref),
                (wp_hbm, wp_ref),
                (bias_hbm, bias_ref),
            )
        )
    ]
    for copy in inputs[:2]:
        copy.start()

    barrier = pltpu.get_barrier_semaphore()
    for dx, dy, dz in offsets:
        pl.semaphore_signal(
            barrier,
            inc=1,
            device_id=device(step_by(x, dx), step_by(y, dy), step_by(z, dz), k),
            device_id_type=MESH,
        )
    mate = device(x, y, z, 1 - k)
    pl.semaphore_signal(barrier, inc=1, device_id=mate, device_id_type=MESH)

    inputs[0].wait()
    inputs[1].wait()
    for copy in inputs[2:]:
        copy.start()
    part = total_rows // CHUNKS
    for i in range(CHUNKS):
        pltpu.make_async_copy(
            table_hbm.at[pl.ds(i * part, part)], table.at[pl.ds(i * part, part)], table_sem
        ).start()

    idx = index_ref[...]
    lane = lax.broadcasted_iota(I32, (samples, lanes), 1)
    table_of = lane // slots_bag
    spread = jnp.where(
        lax.broadcasted_iota(I32, (nt, lanes), 1) // slots_bag == lax.broadcasted_iota(I32, (nt, lanes), 0),
        1.0,
        0.0,
    )
    length = lax.dot_general(
        length_ref[...].astype(F32).astype(BF16),
        spread.astype(BF16),
        (((0,), (0,)), ((), ())),
        preferred_element_type=F32,
    ).astype(I32)
    live = lane - table_of * slots_bag < length
    owner = idx // local_rows
    row = table_of * local_rows + idx - owner * local_rows
    bag = table_of * samples + lax.broadcasted_iota(I32, (samples, lanes), 0)
    owner = jnp.where(live, (owner % 2) * CHIPS + owner // 2, -1)
    pieces = []
    shift = 0
    while shift == 0 or (total_rows - 1) >> shift:
        pieces.append((row // (1 << shift)) % 256)
        shift += 8
    n_row = len(pieces)
    pieces.append(bag + 1)
    pieces = [v.astype(F32) for v in pieces]
    dev_iota = lax.broadcasted_iota(I32, (n, lanes), 0)
    before = (
        lax.broadcasted_iota(I32, (lanes, lanes), 0) < lax.broadcasted_iota(I32, (lanes, lanes), 1)
    )
    before = jnp.where(before, 1.0, 0.0).astype(BF16)
    hots = [
        jnp.where(owner[b : b + 1, :] == dev_iota, 1.0, 0.0).astype(F32) for b in range(samples)
    ]
    prefix = jnp.dot(
        jnp.concatenate([h.astype(BF16) for h in hots], axis=0), before, preferred_element_type=F32
    )
    base = jnp.zeros((n, 1), F32)
    box = jnp.zeros((len(pieces) * n, cap), F32)
    cap_iota = lax.broadcasted_iota(I32, (cap, lanes), 0)
    for b in range(samples):
        hot = hots[b]
        rank = jnp.sum(hot * (prefix[b * n : (b + 1) * n, :] + base), axis=0, keepdims=True)
        base = base + jnp.sum(hot, axis=1, keepdims=True)
        spot = jnp.where(rank.astype(I32) == cap_iota, 1.0, 0.0).astype(BF16)
        coded = jnp.concatenate([hot * v[b : b + 1, :] for v in pieces], axis=0).astype(BF16)
        box = box + lax.dot_general(
            coded, spot, (((1,), (1,)), ((), ())), preferred_element_type=F32
        )
    box_row = jnp.zeros((n, cap), I32)
    for i in range(n_row):
        box_row = box_row + box[i * n : (i + 1) * n, :].astype(I32) * (1 << (8 * i))
    box_bag = box[n_row * n :, :].astype(I32) - 1
    flip = jnp.full((CHIPS, cap), k, I32) == 1
    halves = []
    for both in (box_bag, box_row):
        halves.append(jnp.where(flip, both[CHIPS:], both[:CHIPS]))
        halves.append(jnp.where(flip, both[:CHIPS], both[CHIPS:]))
    boxes = jnp.concatenate(halves, axis=1)
    for d in range(CHIPS):
        outbox[d] = boxes[d : d + 1, :]

    def chip(xx, yy, zz):
        return (xx * SIDE + zz) * SIDE + yy

    inbox[CHIPS - 1] = outbox[chip(x, y, z)]

    pl.semaphore_wait(barrier, CHIPS)

    def slot_of(dx, dy, dz):
        return ((dz - 1) % SIDE * SIDE + (dy - 1) % SIDE) * SIDE + (dx - 1) % SIDE

    for dx, dy, dz in offsets:
        xx, yy, zz = step_by(x, SIDE - dx), step_by(y, SIDE - dy), step_by(z, SIDE - dz)
        pltpu.make_async_remote_copy(
            src_ref=outbox.at[chip(xx, yy, zz)],
            dst_ref=inbox.at[slot_of(dx, dy, dz)],
            send_sem=box_send,
            recv_sem=box_recv,
            device_id=device(xx, yy, zz, k),
            device_id_type=MESH,
        ).start()

    for copy in inputs[2:]:
        copy.wait()
    hidden[...] = (
        jnp.dot(
            dense_ref[...], wd[...], precision=lax.Precision.HIGHEST, preferred_element_type=F32
        )
        + bias_ref[...]
    )

    rest = pl.ds(0, CHIPS - 1)
    boxes_moved = pltpu.make_async_remote_copy(
        src_ref=outbox.at[rest],
        dst_ref=inbox.at[rest],
        send_sem=box_send,
        recv_sem=box_recv,
        device_id=mate,
        device_id_type=MESH,
    )
    boxes_moved.wait_recv()
    forward = pltpu.make_async_remote_copy(
        src_ref=inbox,
        dst_ref=matebox,
        send_sem=fwd_send,
        recv_sem=fwd_recv,
        device_id=mate,
        device_id_type=MESH,
    )
    forward.start()
    own_copy = pltpu.make_async_copy(inbox, ids_own, own_sem)
    own_copy.start()
    forward.wait_recv()

    def mate_copy(q):
        some = pl.ds(q * (CHIPS // SIDE), CHIPS // SIDE)
        return pltpu.make_async_copy(matebox.at[some], ids_mate.at[some], mate_sem.at[q])

    for q in range(SIDE):
        mate_copy(q).start()
    pltpu.make_async_copy(table_hbm, table, table_sem).wait()
    own_copy.wait()

    def inside(at):
        return at & (total_rows - 1)

    def rows_copy(s):
        some = pl.ds(s * SIDE, SIDE)
        return pltpu.make_async_remote_copy(
            src_ref=mate_out.at[some],
            dst_ref=rows_all.at[some, pl.ds(cap, cap)],
            send_sem=rows_send,
            recv_sem=rows_recv.at[s],
            device_id=mate,
            device_id_type=MESH,
        )

    def fetch_mate(s):
        for u in range(SIDE):
            t = s * SIDE + u
            for i in range(cap):
                mate_out[t, i : i + 1, :] = table[pl.ds(inside(ids_mate[t, 0, 3 * cap + i]), 1), :]
        rows_copy(s).start()

    bag_iota = lax.broadcasted_iota(I32, (bags, 2 * cap), 0)

    def a_copy(t, p, to, recv):
        rows = pl.ds(CUT[p], CUT[p + 1] - CUT[p])
        return pltpu.make_async_remote_copy(
            src_ref=a_out.at[t, rows],
            dst_ref=a_in.at[t, rows],
            send_sem=a_send,
            recv_sem=recv,
            device_id=to,
            device_id_type=MESH,
        )

    def b_copy(g, p, to):
        rows = pl.ds(CUT[p], CUT[p + 1] - CUT[p])
        return pltpu.make_async_remote_copy(
            src_ref=b_out.at[g, rows],
            dst_ref=b_in.at[g, rows],
            send_sem=b_send,
            recv_sem=b_recv,
            device_id=to,
            device_id_type=MESH,
        )

    def arrived(slots, p, sem):
        rows = pl.ds(CUT[p], CUT[p + 1] - CUT[p])
        pltpu.make_async_remote_copy(
            src_ref=a_in.at[slots, rows],
            dst_ref=a_in.at[slots, rows],
            send_sem=a_send,
            recv_sem=sem,
            device_id=mate,
            device_id_type=MESH,
        ).wait_recv()

    def pass_on(g, p, slots, to, last):
        lo, hi = CUT[p], CUT[p + 1]
        total = a_in[slots[0], lo:hi, :]
        for t in slots[1:]:
            total = total + a_in[t, lo:hi, :]
        if last is None:
            b_out[g, lo:hi, :] = total
            b_copy(g, p, to).start()
            return

        @pl.when(jnp.logical_not(last))
        def _():
            b_out[g, lo:hi, :] = total
            b_copy(g, p, to).start()

        @pl.when(last)
        def _():
            b_in[g, lo:hi, :] = total

    groups = CHIPS // SIDE

    def step(it, carry):
        @pl.when(it < groups)
        def _():
            @pl.when(it % SIDE == 0)
            def _():
                mate_copy(it // SIDE).wait()

            fetch_mate(it)

        s = it - AHEAD

        @pl.when((s >= 0) & (s < groups))
        def _():
            v, w = s % SIDE, s // SIDE
            rows_copy(s).wait_recv()
            yy, zz = step_by(y, v + 1), step_by(z, w + 1)
            for u in range(SIDE):
                t = s * SIDE + u
                for i in range(cap):
                    rows_all[t, i : i + 1, :] = table[pl.ds(inside(ids_own[t, 0, 2 * cap + i]), 1), :]
            for u in range(SIDE):
                t = s * SIDE + u
                found = rows_all[t]
                high = found.astype(BF16)
                low = (found - high.astype(F32)).astype(BF16)
                select = jnp.where(inbox[t, 0:1, 0 : 2 * cap] == bag_iota, 1.0, 0.0).astype(BF16)
                a_out[t] = jnp.dot(select, high, preferred_element_type=F32) + jnp.dot(
                    select, low, preferred_element_type=F32
                )
            for u in range(SIDE):
                t = s * SIDE + u
                if u < SIDE - 1:
                    a_copy(t, 0, device(step_by(x, u + 1), y, z, k), x_recv.at[s]).start()
                else:
                    a_in[t, CUT[0] : CUT[1], :] = a_out[t, CUT[0] : CUT[1], :]

            @pl.when(v < SIDE - 1)
            def _():
                for u in range(SIDE):
                    a_copy(s * SIDE + u, 1, device(x, yy, z, k), y_recv.at[w]).start()

            @pl.when(v == SIDE - 1)
            def _():
                for u in range(SIDE):
                    t = s * SIDE + u
                    a_in[t, CUT[1] : CUT[2], :] = a_out[t, CUT[1] : CUT[2], :]

            @pl.when(w < SIDE - 1)
            def _():
                for u in range(SIDE):
                    a_copy(s * SIDE + u, 2, device(x, y, zz, k), z_recv).start()

            @pl.when(w == SIDE - 1)
            def _():
                for u in range(SIDE):
                    t = s * SIDE + u
                    a_in[t, CUT[2] : CUT[3], :] = a_out[t, CUT[2] : CUT[3], :]

        j = s - LAG

        @pl.when(j >= 0)
        def _():
            arrived(pl.ds(j * SIDE, SIDE - 1), 0, x_recv.at[j])
            to = device(x, step_by(y, j % SIDE + 1), step_by(z, j // SIDE + 1), k)
            pass_on(j, 0, [j * SIDE + u for u in range(SIDE)], to, j == groups - 1)

        @pl.when((j >= 0) & (j % SIDE == SIDE - 1))
        def _():
            w = j // SIDE
            arrived(pl.ds(w * groups, groups - SIDE), 1, y_recv.at[w])
            for u in range(SIDE):
                to = device(step_by(x, u + 1), y, step_by(z, w + 1), k)
                slots = [w * groups + v * SIDE + u for v in range(SIDE)]
                pass_on(w * SIDE + u, 1, slots, to, w == SIDE - 1 if u == SIDE - 1 else None)

        @pl.when(j == groups - SIDE)
        def _():
            arrived(pl.ds(0, CHIPS - groups), 2, z_recv)

        @pl.when(j >= groups - SIDE)
        def _():
            v = j - (groups - SIDE)
            for u in range(SIDE):
                to = device(step_by(x, u + 1), step_by(y, v + 1), z, k)
                slots = [w * groups + v * SIDE + u for w in range(SIDE)]
                pass_on(v * SIDE + u, 2, slots, to, v == SIDE - 1 if u == SIDE - 1 else None)

        return carry

    lax.fori_loop(0, groups + AHEAD + LAG, step, 0)

    some = pl.ds(0, groups - 1)
    b_moved = pltpu.make_async_remote_copy(
        src_ref=b_out.at[some],
        dst_ref=b_in.at[some],
        send_sem=b_send,
        recv_sem=b_recv,
        device_id=mate,
        device_id_type=MESH,
    )
    b_moved.wait_recv()
    pooled = b_in[0]
    for g in range(1, groups):
        pooled = pooled + b_in[g]

    feats = [dense_ref[...]]
    for t in range(nt):
        feats.append(pooled[t * samples : (t + 1) * samples, :])
        pooled_ref[:, t, :] = feats[-1]
    total = hidden[...]
    pair = 0
    for one in range(nt + 1):
        for two in range(one + 1, nt + 1):
            dots = jnp.sum(feats[one] * feats[two], axis=-1, keepdims=True)
            total = total + dots * wp_ref[pair : pair + 1, :]
            pair += 1
    hidden_ref[...] = jnp.maximum(total, 0.0)

    boxes_moved.wait_send()
    forward.wait_send()
    pltpu.make_async_remote_copy(
        src_ref=mate_out,
        dst_ref=mate_out,
        send_sem=rows_send,
        recv_sem=b_recv,
        device_id=mate,
        device_id_type=MESH,
    ).wait_send()
    some = pl.ds(0, CHIPS - groups)
    pltpu.make_async_remote_copy(
        src_ref=a_out.at[some],
        dst_ref=a_in.at[some],
        send_sem=a_send,
        recv_sem=b_recv,
        device_id=mate,
        device_id_type=MESH,
    ).wait_send()
    b_moved.wait_send()


def shards(bag_index, bag_length, emb_tables, dense_feats, w_dense, w_pair, top_bias):
    samples, lanes = bag_index.shape
    nt, local_rows, width = emb_tables.shape
    cap = 2 * samples * lanes // (2 * CHIPS)
    bags = samples * nt
    units = w_dense.shape[1]
    groups = CHIPS // SIDE
    dims = (local_rows, nt, lanes // nt, cap)
    vmem = pl.BlockSpec(memory_space=pltpu.VMEM)
    anyw = pl.BlockSpec(memory_space=pl.ANY)
    dma = pltpu.SemaphoreType.DMA
    return pl.pallas_call(
        functools.partial(kernel, dims),
        out_shape=(
            jax.ShapeDtypeStruct((samples, nt, width), F32),
            jax.ShapeDtypeStruct((samples, units), F32),
        ),
        in_specs=[anyw] * 7,
        out_specs=(vmem, vmem),
        scratch_shapes=[
            pltpu.VMEM((samples, lanes), I32),
            pltpu.VMEM((nt, samples), I32),
            pltpu.VMEM((samples, width), F32),
            pltpu.VMEM(w_pair.shape, F32),
            pltpu.VMEM((1, units), F32),
            pltpu.VMEM((nt * local_rows, width), F32),
            pltpu.VMEM(w_dense.shape, F32),
            pltpu.VMEM((samples, units), F32),
            pltpu.VMEM((CHIPS, 1, 4 * cap), I32),
            pltpu.VMEM((CHIPS, 1, 4 * cap), I32),
            pltpu.VMEM((CHIPS, 1, 4 * cap), I32),
            pltpu.SMEM((CHIPS, 1, 4 * cap), I32),
            pltpu.SMEM((CHIPS, 1, 4 * cap), I32),
            pltpu.VMEM((CHIPS, cap, width), F32),
            pltpu.VMEM((CHIPS, 2 * cap, width), F32),
            pltpu.VMEM((CHIPS, bags, width), F32),
            pltpu.VMEM((CHIPS, bags, width), F32),
            pltpu.VMEM((groups, bags, width), F32),
            pltpu.VMEM((groups, bags, width), F32),
            dma((6,)),
            dma,
            dma,
            dma,
            dma,
            dma,
            dma,
            dma((SIDE,)),
            dma,
            dma((groups,)),
            dma,
            dma((groups,)),
            dma((SIDE,)),
            dma,
            dma,
            dma,
        ],
        compiler_params=pltpu.CompilerParams(
            collective_id=0, has_side_effects=True, vmem_limit_bytes=60 * 1024 * 1024
        ),
    )(
        bag_index,
        bag_length.T,
        emb_tables.reshape(nt * local_rows, width),
        dense_feats,
        w_dense,
        w_pair,
        top_bias.reshape(1, units),
    )


def solution(mesh):
    in_specs = (
        P(("rows", "cols"), None),
        P(("rows", "cols"), None),
        P(None, ("rows", "cols"), None),
        P(("rows", "cols"), None),
        P(),
        P(),
        P(),
    )
    out_specs = (P(("rows", "cols"), None, None), P(("rows", "cols"), None))
    return jax.shard_map(
        shards, mesh=mesh, in_specs=in_specs, out_specs=out_specs, check_vma=False
    )
```

```python
import functools

import jax
import jax.numpy as jnp
from jax import lax
from jax.experimental import pallas as pl
from jax.experimental.pallas import tpu as pltpu
from jax.sharding import PartitionSpec as P

MESH = pl.DeviceIdType.MESH
F32 = jnp.float32
BF16 = jnp.bfloat16
I32 = jnp.int32
SIDE = 4
CHIPS = SIDE**3
CHUNKS = 8
AHEAD = 5
Z_AT = 9
CUT = (0, 24, 48, 64)


def kernel(
    dims,
    index_hbm,
    length_hbm,
    table_hbm,
    dense_hbm,
    wd_hbm,
    bias_hbm,
    sums_ref,
    start_ref,
    index_ref,
    length_ref,
    dense_ref,
    bias_ref,
    table,
    wd,
    outbox,
    inbox,
    want,
    matebox,
    ids_own,
    ids_mate,
    mate_out,
    own_rows,
    mate_rows,
    a_out,
    a_in,
    b_out,
    b_in,
    input_sem,
    table_sem,
    box_send,
    box_recv,
    fwd_send,
    fwd_recv,
    own_sem,
    mate_sem,
    rows_send,
    rows_recv,
    a_send,
    x_recv,
    y_recv,
    z_recv,
    b_send,
    b_recv,
):
    local_rows, nt, slots_bag, cap = dims
    n = 2 * CHIPS
    samples, lanes = index_ref.shape
    bags = samples * nt
    total_rows = nt * local_rows
    r = lax.axis_index("rows")
    c = lax.axis_index("cols")
    x, z, y, k = r // SIDE, r % SIDE, c // 2, c % 2

    def step_by(at, d):
        return (at + d) % SIDE

    def device(xx, yy, zz, kk):
        return {"rows": xx * SIDE + zz, "cols": yy * 2 + kk}

    offsets = [
        (dx, dy, dz) for dz in range(SIDE) for dy in range(SIDE) for dx in range(SIDE) if dx or dy or dz
    ]
    offsets.sort(key=lambda o: -sum(min(d, SIDE - d) for d in o))

    def far_first(v):
        return (2 + 3 * v + 3 * (v * (v - 1) // 2)) % SIDE

    inputs = [
        pltpu.make_async_copy(source, target, input_sem.at[i])
        for i, (source, target) in enumerate(
            (
                (index_hbm, index_ref),
                (length_hbm, length_ref),
                (wd_hbm, wd),
                (dense_hbm, dense_ref),
                (bias_hbm, bias_ref),
            )
        )
    ]
    for copy in inputs[:2]:
        copy.start()

    barrier = pltpu.get_barrier_semaphore()
    for dx, dy, dz in offsets:
        pl.semaphore_signal(
            barrier,
            inc=1,
            device_id=device(step_by(x, dx), step_by(y, dy), step_by(z, dz), k),
            device_id_type=MESH,
        )
    mate = device(x, y, z, 1 - k)
    pl.semaphore_signal(barrier, inc=1, device_id=mate, device_id_type=MESH)

    inputs[0].wait()
    inputs[1].wait()
    for copy in inputs[2:]:
        copy.start()
    part = total_rows // CHUNKS
    for i in range(CHUNKS):
        pltpu.make_async_copy(
            table_hbm.at[pl.ds(i * part, part)], table.at[pl.ds(i * part, part)], table_sem
        ).start()

    idx = index_ref[...]
    lane = lax.broadcasted_iota(I32, (samples, lanes), 1)
    table_of = lane // slots_bag
    spread = jnp.where(
        lax.broadcasted_iota(I32, (nt, lanes), 1) // slots_bag == lax.broadcasted_iota(I32, (nt, lanes), 0),
        1.0,
        0.0,
    )
    length = lax.dot_general(
        length_ref[...].astype(F32).astype(BF16),
        spread.astype(BF16),
        (((0,), (0,)), ((), ())),
        preferred_element_type=F32,
    ).astype(I32)
    live = lane - table_of * slots_bag < length
    owner = idx // local_rows
    row = table_of * local_rows + idx - owner * local_rows
    bag = table_of * samples + lax.broadcasted_iota(I32, (samples, lanes), 0)
    owner = jnp.where(live, (owner % 2) * CHIPS + owner // 2, -1)
    pieces = []
    shift = 0
    while shift == 0 or (total_rows - 1) >> shift:
        pieces.append((row // (1 << shift)) % 256)
        shift += 8
    n_row = len(pieces)
    pieces.append(bag + 1)
    pieces = [v.astype(F32) for v in pieces]
    dev_iota = lax.broadcasted_iota(I32, (n, lanes), 0)
    before = (
        lax.broadcasted_iota(I32, (lanes, lanes), 0) < lax.broadcasted_iota(I32, (lanes, lanes), 1)
    )
    before = jnp.where(before, 1.0, 0.0).astype(BF16)
    hots = [
        jnp.where(owner[b : b + 1, :] == dev_iota, 1.0, 0.0).astype(F32) for b in range(samples)
    ]
    prefix = jnp.dot(
        jnp.concatenate([h.astype(BF16) for h in hots], axis=0), before, preferred_element_type=F32
    )
    base = jnp.zeros((n, 1), F32)
    box = jnp.zeros((len(pieces) * n, cap), F32)
    cap_iota = lax.broadcasted_iota(I32, (cap, lanes), 0)
    for b in range(samples):
        hot = hots[b]
        rank = jnp.sum(hot * (prefix[b * n : (b + 1) * n, :] + base), axis=0, keepdims=True)
        base = base + jnp.sum(hot, axis=1, keepdims=True)
        spot = jnp.where(rank.astype(I32) == cap_iota, 1.0, 0.0).astype(BF16)
        coded = jnp.concatenate([hot * v[b : b + 1, :] for v in pieces], axis=0).astype(BF16)
        box = box + lax.dot_general(
            coded, spot, (((1,), (1,)), ((), ())), preferred_element_type=F32
        )
    box_row = jnp.zeros((n, cap), I32)
    for i in range(n_row):
        box_row = box_row + box[i * n : (i + 1) * n, :].astype(I32) * (1 << (8 * i))
    box_bag = box[n_row * n :, :].astype(I32) - 1
    flip = jnp.full((CHIPS, cap), k, I32) == 1
    halves = []
    for both in (box_bag, box_row):
        halves.append(jnp.where(flip, both[CHIPS:], both[:CHIPS]))
        halves.append(jnp.where(flip, both[:CHIPS], both[CHIPS:]))
    boxes = jnp.concatenate(halves, axis=1)
    for d in range(CHIPS):
        outbox[d] = boxes[d : d + 1, :]

    def chip(xx, yy, zz):
        return (xx * SIDE + zz) * SIDE + yy

    inbox[CHIPS - 1] = outbox[chip(x, y, z)]

    pl.semaphore_wait(barrier, CHIPS)

    def slot_of(dx, dy, dz):
        place = [far_first(v) for v in range(SIDE)]
        return (place.index(dz) * SIDE + place.index(dy)) * SIDE + place.index(dx)

    for dx, dy, dz in offsets:
        xx, yy, zz = step_by(x, SIDE - dx), step_by(y, SIDE - dy), step_by(z, SIDE - dz)
        pltpu.make_async_remote_copy(
            src_ref=outbox.at[chip(xx, yy, zz)],
            dst_ref=inbox.at[slot_of(dx, dy, dz)],
            send_sem=box_send,
            recv_sem=box_recv,
            device_id=device(xx, yy, zz, k),
            device_id_type=MESH,
        ).start()

    for copy in inputs[2:]:
        copy.wait()
    start_ref[...] = (
        jnp.dot(
            dense_ref[...], wd[...], precision=lax.Precision.HIGHEST, preferred_element_type=F32
        )
        + bias_ref[...]
    )

    rest = pl.ds(0, CHIPS - 1)
    boxes_moved = pltpu.make_async_remote_copy(
        src_ref=outbox.at[rest],
        dst_ref=inbox.at[rest],
        send_sem=box_send,
        recv_sem=box_recv,
        device_id=mate,
        device_id_type=MESH,
    )
    boxes_moved.wait_recv()
    want[...] = inbox[...] & (total_rows - 1)
    forward = pltpu.make_async_remote_copy(
        src_ref=want,
        dst_ref=matebox,
        send_sem=fwd_send,
        recv_sem=fwd_recv,
        device_id=mate,
        device_id_type=MESH,
    )
    forward.start()
    own_copy = pltpu.make_async_copy(want, ids_own, own_sem)
    own_copy.start()
    forward.wait_recv()

    def mate_copy(q):
        some = pl.ds(q * (CHIPS // SIDE), CHIPS // SIDE)
        return pltpu.make_async_copy(matebox.at[some], ids_mate.at[some], mate_sem.at[q])

    for q in range(SIDE):
        mate_copy(q).start()
    pltpu.make_async_copy(table_hbm, table, table_sem).wait()
    own_copy.wait()

    def rows_copy(s):
        some = pl.ds(s * SIDE, SIDE)
        return pltpu.make_async_remote_copy(
            src_ref=mate_out.at[some],
            dst_ref=mate_rows.at[some],
            send_sem=rows_send,
            recv_sem=rows_recv.at[s],
            device_id=mate,
            device_id_type=MESH,
        )

    def fetch_mate(s):
        for u in range(SIDE):
            t = s * SIDE + u
            for i in range(cap):
                mate_out[t, i : i + 1, :] = table[pl.ds(ids_mate[t, 0, 3 * cap + i], 1), :]
        rows_copy(s).start()

    def fetch_own(s):
        for u in range(SIDE):
            t = s * SIDE + u
            for i in range(cap):
                own_rows[u, i : i + 1, :] = table[pl.ds(ids_own[t, 0, 2 * cap + i], 1), :]

    for s in range(AHEAD):
        if s % SIDE == 0:
            mate_copy(s // SIDE).wait()
        fetch_mate(s)
    fetch_own(0)
    for q in range((AHEAD + SIDE - 1) // SIDE, SIDE):
        mate_copy(q).wait()

    bag_iota = lax.broadcasted_iota(I32, (bags, 2 * cap), 0)

    def a_copy(slots, p, to, recv):
        rows = pl.ds(CUT[p], CUT[p + 1] - CUT[p])
        return pltpu.make_async_remote_copy(
            src_ref=a_out.at[slots, rows],
            dst_ref=a_in.at[slots, rows],
            send_sem=a_send,
            recv_sem=recv,
            device_id=to,
            device_id_type=MESH,
        )

    def b_copy(g, p, to):
        rows = pl.ds(CUT[p], CUT[p + 1] - CUT[p])
        return pltpu.make_async_remote_copy(
            src_ref=b_out.at[g, rows],
            dst_ref=b_in.at[g, rows],
            send_sem=b_send,
            recv_sem=b_recv,
            device_id=to,
            device_id_type=MESH,
        )

    def arrived(slots, p, sem):
        rows = pl.ds(CUT[p], CUT[p + 1] - CUT[p])
        pltpu.make_async_remote_copy(
            src_ref=a_in.at[slots, rows],
            dst_ref=a_in.at[slots, rows],
            send_sem=a_send,
            recv_sem=sem,
            device_id=mate,
            device_id_type=MESH,
        ).wait_recv()

    def pass_on(g, p, slots, to, last):
        lo, hi = CUT[p], CUT[p + 1]
        total = a_in[slots[0], lo:hi, :]
        for t in slots[1:]:
            total = total + a_in[t, lo:hi, :]
        if last is None:
            b_out[g, lo:hi, :] = total
            b_copy(g, p, to).start()
            return

        @pl.when(jnp.logical_not(last))
        def _():
            b_out[g, lo:hi, :] = total
            b_copy(g, p, to).start()

        @pl.when(last)
        def _():
            b_in[g, lo:hi, :] = total

    groups = CHIPS // SIDE

    def keep_own(s, p):
        lo, hi = CUT[p], CUT[p + 1]
        for u in range(SIDE):
            t = s * SIDE + u
            a_in[t, lo:hi, :] = a_out[t, lo:hi, :]

    def pool(s, more):
        v, w = s % SIDE, s // SIDE
        rows_copy(s).wait_recv()
        for u in range(SIDE):
            t = s * SIDE + u
            found = jnp.concatenate([own_rows[u], mate_rows[t]], axis=0)
            high = found.astype(BF16)
            low = (found - high.astype(F32)).astype(BF16)
            select = jnp.where(want[t, 0:1, 0 : 2 * cap] == bag_iota, 1.0, 0.0).astype(BF16)
            value = jnp.dot(select, high, preferred_element_type=F32) + jnp.dot(
                select, low, preferred_element_type=F32
            )
            a_out[t] = value
            if u == SIDE - 1:
                a_in[t, CUT[0] : CUT[1], :] = value[CUT[0] : CUT[1]]
        if more:
            fetch_own(s + 1)
            fetch_mate(s + AHEAD)
        else:
            fetch_own(jnp.minimum(s + 1, groups - 1))
        for u in range(SIDE - 1):
            to = device(step_by(x, far_first(u)), y, z, k)
            a_copy(pl.ds(s * SIDE + u, 1), 0, to, x_recv.at[s]).start()
        four = pl.ds(s * SIDE, SIDE)

        @pl.when(v < SIDE - 1)
        def _():
            a_copy(four, 1, device(x, step_by(y, far_first(v)), z, k), y_recv.at[w]).start()

        @pl.when(w < SIDE - 1)
        def _():
            a_copy(four, 2, device(x, y, step_by(z, far_first(w)), k), z_recv).start()

        @pl.when(v == SIDE - 1)
        def _():
            keep_own(s, 1)

        @pl.when(w == SIDE - 1)
        def _():
            keep_own(s, 2)

    def reduce(j, carry):
        i = j - Z_AT

        @pl.when(i == 0)
        def _():
            arrived(pl.ds(0, CHIPS - groups), 2, z_recv)

        @pl.when((i >= 0) & (i < SIDE))
        def _():
            for u in range(SIDE):
                to = device(step_by(x, far_first(u)), step_by(y, far_first(i)), z, k)
                slots = [w * groups + i * SIDE + u for w in range(SIDE)]
                pass_on(i * SIDE + u, 2, slots, to, i == SIDE - 1 if u == SIDE - 1 else None)

        arrived(pl.ds(j * SIDE, SIDE - 1), 0, x_recv.at[j])
        to = device(x, step_by(y, far_first(j % SIDE)), step_by(z, far_first(j // SIDE)), k)
        pass_on(j, 0, [j * SIDE + u for u in range(SIDE)], to, j == groups - 1)

        @pl.when(j % SIDE == SIDE - 1)
        def _():
            w = j // SIDE
            arrived(pl.ds(w * groups, groups - SIDE), 1, y_recv.at[w])
            for u in range(SIDE):
                to = device(step_by(x, far_first(u)), y, step_by(z, far_first(w)), k)
                slots = [w * groups + v * SIDE + u for v in range(SIDE)]
                pass_on(w * SIDE + u, 1, slots, to, w == SIDE - 1 if u == SIDE - 1 else None)

        return carry

    def step_full(s, carry):
        pool(s, True)
        return carry

    def step_last(s, carry):
        pool(s, False)
        return carry

    lax.fori_loop(0, groups - AHEAD, step_full, 0)
    lax.fori_loop(groups - AHEAD, groups, step_last, 0)
    lax.fori_loop(0, groups, reduce, 0)

    some = pl.ds(0, groups - 1)
    b_moved = pltpu.make_async_remote_copy(
        src_ref=b_out.at[some],
        dst_ref=b_in.at[some],
        send_sem=b_send,
        recv_sem=b_recv,
        device_id=mate,
        device_id_type=MESH,
    )
    b_moved.wait_recv()
    pooled = b_in[0]
    for g in range(1, groups):
        pooled = pooled + b_in[g]

    sums_ref[...] = pooled

    boxes_moved.wait_send()
    forward.wait_send()
    pltpu.make_async_remote_copy(
        src_ref=mate_out,
        dst_ref=mate_out,
        send_sem=rows_send,
        recv_sem=b_recv,
        device_id=mate,
        device_id_type=MESH,
    ).wait_send()
    some = pl.ds(0, CHIPS - groups)
    pltpu.make_async_remote_copy(
        src_ref=a_out.at[some],
        dst_ref=a_in.at[some],
        send_sem=a_send,
        recv_sem=b_recv,
        device_id=mate,
        device_id_type=MESH,
    ).wait_send()
    b_moved.wait_send()


def interact(sums_ref, start_ref, dense_ref, wp_ref, pooled_ref, hidden_ref):
    samples, nt = pooled_ref.shape[0], pooled_ref.shape[1]
    pooled = sums_ref[...]
    feats = [dense_ref[...]]
    for t in range(nt):
        feats.append(pooled[t * samples : (t + 1) * samples, :])
        pooled_ref[:, t, :] = feats[-1]
    total = start_ref[...]
    pair = 0
    for one in range(nt + 1):
        for two in range(one + 1, nt + 1):
            dots = jnp.sum(feats[one] * feats[two], axis=-1, keepdims=True)
            total = total + dots * wp_ref[pair : pair + 1, :]
            pair += 1
    hidden_ref[...] = jnp.maximum(total, 0.0)


def shards(bag_index, bag_length, emb_tables, dense_feats, w_dense, w_pair, top_bias):
    samples, lanes = bag_index.shape
    nt, local_rows, width = emb_tables.shape
    cap = 2 * samples * lanes // (2 * CHIPS)
    bags = samples * nt
    units = w_dense.shape[1]
    groups = CHIPS // SIDE
    dims = (local_rows, nt, lanes // nt, cap)
    vmem = pl.BlockSpec(memory_space=pltpu.VMEM)
    anyw = pl.BlockSpec(memory_space=pl.ANY)
    dma = pltpu.SemaphoreType.DMA
    sums, start = pl.pallas_call(
        functools.partial(kernel, dims),
        out_shape=(
            jax.ShapeDtypeStruct((bags, width), F32),
            jax.ShapeDtypeStruct((samples, units), F32),
        ),
        in_specs=[anyw] * 6,
        out_specs=(vmem, vmem),
        scratch_shapes=[
            pltpu.VMEM((samples, lanes), I32),
            pltpu.VMEM((nt, samples), I32),
            pltpu.VMEM((samples, width), F32),
            pltpu.VMEM((1, units), F32),
            pltpu.VMEM((nt * local_rows, width), F32),
            pltpu.VMEM(w_dense.shape, F32),
            pltpu.VMEM((CHIPS, 1, 4 * cap), I32),
            pltpu.VMEM((CHIPS, 1, 4 * cap), I32),
            pltpu.VMEM((CHIPS, 1, 4 * cap), I32),
            pltpu.VMEM((CHIPS, 1, 4 * cap), I32),
            pltpu.SMEM((CHIPS, 1, 4 * cap), I32),
            pltpu.SMEM((CHIPS, 1, 4 * cap), I32),
            pltpu.VMEM((CHIPS, cap, width), F32),
            pltpu.VMEM((SIDE, cap, width), F32),
            pltpu.VMEM((CHIPS, cap, width), F32),
            pltpu.VMEM((CHIPS, bags, width), F32),
            pltpu.VMEM((CHIPS, bags, width), F32),
            pltpu.VMEM((groups, bags, width), F32),
            pltpu.VMEM((groups, bags, width), F32),
            dma((5,)),
            dma,
            dma,
            dma,
            dma,
            dma,
            dma,
            dma((SIDE,)),
            dma,
            dma((groups,)),
            dma,
            dma((groups,)),
            dma((SIDE,)),
            dma,
            dma,
            dma,
        ],
        compiler_params=pltpu.CompilerParams(
            collective_id=0, has_side_effects=True, vmem_limit_bytes=60 * 1024 * 1024
        ),
    )(
        bag_index,
        bag_length.T,
        emb_tables.reshape(nt * local_rows, width),
        dense_feats,
        w_dense,
        top_bias.reshape(1, units),
    )
    return pl.pallas_call(
        interact,
        out_shape=(
            jax.ShapeDtypeStruct((samples, nt, width), F32),
            jax.ShapeDtypeStruct((samples, units), F32),
        ),
        in_specs=[vmem] * 4,
        out_specs=(vmem, vmem),
    )(sums, start, dense_feats, w_pair)


def solution(mesh):
    in_specs = (
        P(("rows", "cols"), None),
        P(("rows", "cols"), None),
        P(None, ("rows", "cols"), None),
        P(("rows", "cols"), None),
        P(),
        P(),
        P(),
    )
    out_specs = (P(("rows", "cols"), None, None), P(("rows", "cols"), None))
    return jax.shard_map(
        shards, mesh=mesh, in_specs=in_specs, out_specs=out_specs, check_vma=False
    )
```

```python
import functools

import jax
import jax.numpy as jnp
from jax import lax
from jax.experimental import pallas as pl
from jax.experimental.pallas import tpu as pltpu
from jax.sharding import PartitionSpec as P

MESH = pl.DeviceIdType.MESH
F32 = jnp.float32
BF16 = jnp.bfloat16
I32 = jnp.int32
SIDE = 4
CHIPS = SIDE**3
CHUNKS = 8
AHEAD = 5
CUT = (0, 24, 48, 64)
FAR = SIDE // 2


def destinations():
    near = [1, 3, 0]
    out = []
    for far in ((1, 1, 1), (1, 1, 0), (1, 0, 1), (0, 1, 1), (1, 0, 0), (0, 1, 0), (0, 0, 1), (0, 0, 0)):
        dims = [[FAR] if f else near for f in far]
        out += [(dx, dy, dz) for dz in dims[2] for dy in dims[1] for dx in dims[0]]
    return out


ORDER = destinations()
SLOT = {d: t for t, d in enumerate(ORDER)}


def others(d, p):
    return tuple(v for q, v in enumerate(d) if q != p)


def along(p, v, o):
    return o[:p] + (v,) + o[p:]


def plane_order():
    near = [1, 3, 0]
    out = [(FAR, FAR)] + [(FAR, b) for b in near] + [(a, FAR) for a in near]
    return out + [(a, b) for b in near for a in near]


PLANE = plane_order()
PLACE = {o: g for g, o in enumerate(PLANE)}
TEAM = [0] * 7 + [1] * 3 + [2] * 3 + [3] * 3
TEAMS = 4


def joined(o):
    return 1 if sum(o) % 2 == 0 else SIDE - 1


def kernel(
    dims,
    index_hbm,
    length_hbm,
    table_hbm,
    dense_hbm,
    wd_hbm,
    bias_hbm,
    sums_ref,
    start_ref,
    index_ref,
    length_ref,
    dense_ref,
    bias_ref,
    table,
    wd,
    outbox,
    inbox,
    want,
    matebox,
    mate_want,
    ids_own,
    ids_mate,
    mate_out,
    own_rows,
    mate_rows,
    a_out,
    a_in,
    b_out,
    b_in,
    input_sem,
    table_sem,
    box_send,
    box_recv,
    fwd_send,
    fwd_recv,
    own_sem,
    mate_sem,
    rows_send,
    rows_recv,
    a_send,
    far_recv,
    near_recv,
    b_send,
    b_recv,
):
    local_rows, nt, slots_bag, cap = dims
    n = 2 * CHIPS
    samples, lanes = index_ref.shape
    bags = samples * nt
    total_rows = nt * local_rows
    r = lax.axis_index("rows")
    c = lax.axis_index("cols")
    x, z, y, k = r // SIDE, r % SIDE, c // 2, c % 2

    def step_by(at, d):
        return (at + d) % SIDE

    def device(xx, yy, zz, kk):
        return {"rows": xx * SIDE + zz, "cols": yy * 2 + kk}

    offsets = sorted(ORDER, key=lambda o: -sum(min(d, SIDE - d) for d in o))

    def shifted(d, kk):
        return device(step_by(x, d[0]), step_by(y, d[1]), step_by(z, d[2]), kk)

    inputs = [
        pltpu.make_async_copy(source, target, input_sem.at[i])
        for i, (source, target) in enumerate(
            (
                (index_hbm, index_ref),
                (length_hbm, length_ref),
                (wd_hbm, wd),
                (dense_hbm, dense_ref),
                (bias_hbm, bias_ref),
            )
        )
    ]
    for copy in inputs[:2]:
        copy.start()

    mate = device(x, y, z, 1 - k)

    barrier = pltpu.get_barrier_semaphore()
    for d in offsets:
        pl.semaphore_signal(barrier, inc=1, device_id=shifted(d, 1 - k), device_id_type=MESH)
        if any(d):
            pl.semaphore_signal(barrier, inc=1, device_id=shifted(d, k), device_id_type=MESH)

    inputs[0].wait()
    inputs[1].wait()
    for copy in inputs[2:]:
        copy.start()
    part = total_rows // CHUNKS
    for i in range(CHUNKS):
        pltpu.make_async_copy(
            table_hbm.at[pl.ds(i * part, part)], table.at[pl.ds(i * part, part)], table_sem
        ).start()

    idx = index_ref[...]
    lane = lax.broadcasted_iota(I32, (samples, lanes), 1)
    table_of = lane // slots_bag
    spread = jnp.where(
        lax.broadcasted_iota(I32, (nt, lanes), 1) // slots_bag == lax.broadcasted_iota(I32, (nt, lanes), 0),
        1.0,
        0.0,
    )
    length = lax.dot_general(
        length_ref[...].astype(F32).astype(BF16),
        spread.astype(BF16),
        (((0,), (0,)), ((), ())),
        preferred_element_type=F32,
    ).astype(I32)
    live = lane - table_of * slots_bag < length
    owner = idx // local_rows
    row = table_of * local_rows + idx - owner * local_rows
    bag = table_of * samples + lax.broadcasted_iota(I32, (samples, lanes), 0)
    owner = jnp.where(live, (owner % 2) * CHIPS + owner // 2, -1)
    pieces = []
    shift = 0
    while shift == 0 or (total_rows - 1) >> shift:
        pieces.append((row // (1 << shift)) % 256)
        shift += 8
    n_row = len(pieces)
    pieces.append(bag + 1)
    pieces = [v.astype(F32) for v in pieces]
    dev_iota = lax.broadcasted_iota(I32, (n, lanes), 0)
    before = (
        lax.broadcasted_iota(I32, (lanes, lanes), 0) < lax.broadcasted_iota(I32, (lanes, lanes), 1)
    )
    before = jnp.where(before, 1.0, 0.0).astype(BF16)
    hots = [
        jnp.where(owner[b : b + 1, :] == dev_iota, 1.0, 0.0).astype(F32) for b in range(samples)
    ]
    prefix = jnp.dot(
        jnp.concatenate([h.astype(BF16) for h in hots], axis=0), before, preferred_element_type=F32
    )
    base = jnp.zeros((n, 1), F32)
    box = jnp.zeros((len(pieces) * n, cap), F32)
    cap_iota = lax.broadcasted_iota(I32, (cap, lanes), 0)
    for b in range(samples):
        hot = hots[b]
        rank = jnp.sum(hot * (prefix[b * n : (b + 1) * n, :] + base), axis=0, keepdims=True)
        base = base + jnp.sum(hot, axis=1, keepdims=True)
        spot = jnp.where(rank.astype(I32) == cap_iota, 1.0, 0.0).astype(BF16)
        coded = jnp.concatenate([hot * v[b : b + 1, :] for v in pieces], axis=0).astype(BF16)
        box = box + lax.dot_general(
            coded, spot, (((1,), (1,)), ((), ())), preferred_element_type=F32
        )
    box_row = jnp.zeros((n, cap), I32)
    for i in range(n_row):
        box_row = box_row + box[i * n : (i + 1) * n, :].astype(I32) * (1 << (8 * i))
    box_bag = box[n_row * n :, :].astype(I32) - 1
    flip = jnp.full((CHIPS, cap), k, I32) == 1
    halves = []
    for both in (box_bag, box_row):
        halves.append(jnp.where(flip, both[CHIPS:], both[:CHIPS]))
        halves.append(jnp.where(flip, both[:CHIPS], both[CHIPS:]))
    boxes = jnp.concatenate(halves, axis=1)
    for d in range(CHIPS):
        outbox[d] = boxes[d : d + 1, :]

    def chip(xx, yy, zz):
        return (xx * SIDE + zz) * SIDE + yy

    inbox[SLOT[(0, 0, 0)]] = outbox[chip(x, y, z)]

    pl.semaphore_wait(barrier, n - 1)

    for d in offsets:
        back = tuple((SIDE - v) % SIDE for v in d)
        source = outbox.at[chip(step_by(x, back[0]), step_by(y, back[1]), step_by(z, back[2]))]
        pltpu.make_async_remote_copy(
            src_ref=source,
            dst_ref=matebox.at[SLOT[d]],
            send_sem=fwd_send,
            recv_sem=fwd_recv,
            device_id=shifted(back, 1 - k),
            device_id_type=MESH,
        ).start()
        if any(d):
            pltpu.make_async_remote_copy(
                src_ref=source,
                dst_ref=inbox.at[SLOT[d]],
                send_sem=box_send,
                recv_sem=box_recv,
                device_id=shifted(back, k),
                device_id_type=MESH,
            ).start()

    for copy in inputs[2:]:
        copy.wait()
    start_ref[...] = (
        jnp.dot(
            dense_ref[...], wd[...], precision=lax.Precision.HIGHEST, preferred_element_type=F32
        )
        + bias_ref[...]
    )

    rest = pl.ds(0, CHIPS - 1)
    boxes_moved = pltpu.make_async_remote_copy(
        src_ref=outbox.at[rest],
        dst_ref=inbox.at[rest],
        send_sem=box_send,
        recv_sem=box_recv,
        device_id=mate,
        device_id_type=MESH,
    )
    mates_moved = pltpu.make_async_remote_copy(
        src_ref=outbox,
        dst_ref=matebox,
        send_sem=fwd_send,
        recv_sem=fwd_recv,
        device_id=mate,
        device_id_type=MESH,
    )
    quarter = CHIPS // SIDE

    def mate_copy(q):
        some = pl.ds(q * quarter, quarter)
        return pltpu.make_async_copy(mate_want.at[some], ids_mate.at[some], mate_sem.at[q])

    mates_moved.wait_recv()
    mate_want[...] = matebox[...] & (total_rows - 1)
    for q in range(SIDE):
        mate_copy(q).start()
    boxes_moved.wait_recv()
    want[...] = inbox[...] & (total_rows - 1)
    own_copy = pltpu.make_async_copy(want, ids_own, own_sem)
    own_copy.start()
    pltpu.make_async_copy(table_hbm, table, table_sem).wait()

    def rows_copy(s):
        some = pl.ds(s * SIDE, SIDE)
        return pltpu.make_async_remote_copy(
            src_ref=mate_out.at[some],
            dst_ref=mate_rows.at[some],
            send_sem=rows_send,
            recv_sem=rows_recv.at[s],
            device_id=mate,
            device_id_type=MESH,
        )

    def fetch_mate(s):
        for u in range(SIDE):
            t = s * SIDE + u
            for i in range(cap):
                mate_out[t, i : i + 1, :] = table[pl.ds(ids_mate[t, 0, 3 * cap + i], 1), :]
        rows_copy(s).start()

    def fetch_own(s):
        for u in range(SIDE):
            t = s * SIDE + u
            for i in range(cap):
                own_rows[u, i : i + 1, :] = table[pl.ds(ids_own[t, 0, 2 * cap + i], 1), :]

    for s in range(AHEAD):
        if s % SIDE == 0:
            mate_copy(s // SIDE).wait()
        fetch_mate(s)
    own_copy.wait()
    fetch_own(0)
    for q in range((AHEAD + SIDE - 1) // SIDE, SIDE):
        mate_copy(q).wait()

    bag_iota = lax.broadcasted_iota(I32, (bags, 2 * cap), 0)

    def rows_of(p):
        return pl.ds(CUT[p], CUT[p + 1] - CUT[p])

    def a_copy(t, p, shift, recv):
        return pltpu.make_async_remote_copy(
            src_ref=a_out.at[t, rows_of(p)],
            dst_ref=a_in.at[t, rows_of(p)],
            send_sem=a_send,
            recv_sem=recv,
            device_id=shifted(along(p, shift, (0, 0)), k),
            device_id_type=MESH,
        )

    def b_copy(g, p):
        return pltpu.make_async_remote_copy(
            src_ref=b_out.at[g, rows_of(p)],
            dst_ref=b_in.at[g, rows_of(p)],
            send_sem=b_send,
            recv_sem=b_recv,
            device_id=shifted(along(p, 0, PLANE[g]), k),
            device_id_type=MESH,
        )

    def arrived(count, p, sem):
        pltpu.make_async_remote_copy(
            src_ref=a_in.at[pl.ds(0, count), rows_of(p)],
            dst_ref=a_in.at[pl.ds(0, count), rows_of(p)],
            send_sem=a_send,
            recv_sem=sem,
            device_id=mate,
            device_id_type=MESH,
        ).wait_recv()

    groups = CHIPS // SIDE

    def pool(s):
        rows_copy(s).wait_recv()
        slots = range(s * SIDE, (s + 1) * SIDE)
        for t in slots:
            found = jnp.concatenate([own_rows[t % SIDE], mate_rows[t]], axis=0)
            high = found.astype(BF16)
            low = (found - high.astype(F32)).astype(BF16)
            select = jnp.where(want[t, 0:1, 0 : 2 * cap] == bag_iota, 1.0, 0.0).astype(BF16)
            value = jnp.dot(select, high, preferred_element_type=F32) + jnp.dot(
                select, low, preferred_element_type=F32
            )
            a_out[t] = value
            for p in range(3):
                if ORDER[t][p] == 0:
                    a_in[t, CUT[p] : CUT[p + 1], :] = value[CUT[p] : CUT[p + 1]]
        if s + 1 < groups:
            fetch_own(s + 1)
        if s + AHEAD < groups:
            fetch_mate(s + AHEAD)
        for t in slots:
            for p in range(3):
                o, v = others(ORDER[t], p), ORDER[t][p]
                team = TEAM[PLACE[o]]
                if v == FAR:
                    a_copy(t, p, joined(o), far_recv.at[p, team]).start()
                elif v and v != joined(o):
                    a_copy(t, p, v, near_recv.at[p, team]).start()

    for s in range(groups):
        pool(s)
    for team in range(TEAMS):
        planes = [o for o in PLANE if TEAM[PLACE[o]] == team]
        for p in range(3):
            lo, hi = CUT[p], CUT[p + 1]
            arrived(len(planes), p, far_recv.at[p, team])
            for o in planes:
                t, far = SLOT[along(p, joined(o), o)], SLOT[along(p, FAR, o)]
                a_out[t, lo:hi, :] = a_out[t, lo:hi, :] + a_in[far, lo:hi, :]
                a_copy(t, p, joined(o), near_recv.at[p, team]).start()
    for team in range(TEAMS):
        planes = [o for o in PLANE if TEAM[PLACE[o]] == team]
        for p in range(3):
            lo, hi = CUT[p], CUT[p + 1]
            arrived(2 * len(planes), p, near_recv.at[p, team])
            for o in planes:
                g = PLACE[o]
                total = a_in[SLOT[along(p, 0, o)], lo:hi, :]
                for v in (1, SIDE - 1):
                    total = total + a_in[SLOT[along(p, v, o)], lo:hi, :]
                if any(o):
                    b_out[g, lo:hi, :] = total
                    b_copy(g, p).start()
                else:
                    b_in[g, lo:hi, :] = total

    some = pl.ds(0, groups - 1)
    b_moved = pltpu.make_async_remote_copy(
        src_ref=b_out.at[some],
        dst_ref=b_in.at[some],
        send_sem=b_send,
        recv_sem=b_recv,
        device_id=mate,
        device_id_type=MESH,
    )
    b_moved.wait_recv()
    pooled = b_in[0]
    for g in range(1, groups):
        pooled = pooled + b_in[g]

    sums_ref[...] = pooled

    boxes_moved.wait_send()
    mates_moved.wait_send()
    pltpu.make_async_remote_copy(
        src_ref=mate_out,
        dst_ref=mate_out,
        send_sem=rows_send,
        recv_sem=b_recv,
        device_id=mate,
        device_id_type=MESH,
    ).wait_send()
    some = pl.ds(0, CHIPS - groups)
    pltpu.make_async_remote_copy(
        src_ref=a_out.at[some],
        dst_ref=a_in.at[some],
        send_sem=a_send,
        recv_sem=b_recv,
        device_id=mate,
        device_id_type=MESH,
    ).wait_send()
    b_moved.wait_send()


def interact(sums_ref, start_ref, dense_ref, wp_ref, pooled_ref, hidden_ref):
    samples, nt = pooled_ref.shape[0], pooled_ref.shape[1]
    pooled = sums_ref[...]
    feats = [dense_ref[...]]
    for t in range(nt):
        feats.append(pooled[t * samples : (t + 1) * samples, :])
        pooled_ref[:, t, :] = feats[-1]
    total = start_ref[...]
    pair = 0
    for one in range(nt + 1):
        for two in range(one + 1, nt + 1):
            dots = jnp.sum(feats[one] * feats[two], axis=-1, keepdims=True)
            total = total + dots * wp_ref[pair : pair + 1, :]
            pair += 1
    hidden_ref[...] = jnp.maximum(total, 0.0)


def shards(bag_index, bag_length, emb_tables, dense_feats, w_dense, w_pair, top_bias):
    samples, lanes = bag_index.shape
    nt, local_rows, width = emb_tables.shape
    cap = 2 * samples * lanes // (2 * CHIPS)
    bags = samples * nt
    units = w_dense.shape[1]
    groups = CHIPS // SIDE
    dims = (local_rows, nt, lanes // nt, cap)
    vmem = pl.BlockSpec(memory_space=pltpu.VMEM)
    anyw = pl.BlockSpec(memory_space=pl.ANY)
    dma = pltpu.SemaphoreType.DMA
    sums, start = pl.pallas_call(
        functools.partial(kernel, dims),
        out_shape=(
            jax.ShapeDtypeStruct((bags, width), F32),
            jax.ShapeDtypeStruct((samples, units), F32),
        ),
        in_specs=[anyw] * 6,
        out_specs=(vmem, vmem),
        scratch_shapes=[
            pltpu.VMEM((samples, lanes), I32),
            pltpu.VMEM((nt, samples), I32),
            pltpu.VMEM((samples, width), F32),
            pltpu.VMEM((1, units), F32),
            pltpu.VMEM((nt * local_rows, width), F32),
            pltpu.VMEM(w_dense.shape, F32),
            pltpu.VMEM((CHIPS, 1, 4 * cap), I32),
            pltpu.VMEM((CHIPS, 1, 4 * cap), I32),
            pltpu.VMEM((CHIPS, 1, 4 * cap), I32),
            pltpu.VMEM((CHIPS, 1, 4 * cap), I32),
            pltpu.VMEM((CHIPS, 1, 4 * cap), I32),
            pltpu.SMEM((CHIPS, 1, 4 * cap), I32),
            pltpu.SMEM((CHIPS, 1, 4 * cap), I32),
            pltpu.VMEM((CHIPS, cap, width), F32),
            pltpu.VMEM((SIDE, cap, width), F32),
            pltpu.VMEM((CHIPS, cap, width), F32),
            pltpu.VMEM((CHIPS, bags, width), F32),
            pltpu.VMEM((CHIPS, bags, width), F32),
            pltpu.VMEM((groups, bags, width), F32),
            pltpu.VMEM((groups, bags, width), F32),
            dma((5,)),
            dma,
            dma,
            dma,
            dma,
            dma,
            dma,
            dma((SIDE,)),
            dma,
            dma((groups,)),
            dma,
            dma((3, TEAMS)),
            dma((3, TEAMS)),
            dma,
            dma,
        ],
        compiler_params=pltpu.CompilerParams(
            collective_id=0, has_side_effects=True, vmem_limit_bytes=60 * 1024 * 1024
        ),
    )(
        bag_index,
        bag_length.T,
        emb_tables.reshape(nt * local_rows, width),
        dense_feats,
        w_dense,
        top_bias.reshape(1, units),
    )
    return pl.pallas_call(
        interact,
        out_shape=(
            jax.ShapeDtypeStruct((samples, nt, width), F32),
            jax.ShapeDtypeStruct((samples, units), F32),
        ),
        in_specs=[vmem] * 4,
        out_specs=(vmem, vmem),
    )(sums, start, dense_feats, w_pair)


def solution(mesh):
    in_specs = (
        P(("rows", "cols"), None),
        P(("rows", "cols"), None),
        P(None, ("rows", "cols"), None),
        P(("rows", "cols"), None),
        P(),
        P(),
        P(),
    )
    out_specs = (P(("rows", "cols"), None, None), P(("rows", "cols"), None))
    return jax.shard_map(
        shards, mesh=mesh, in_specs=in_specs, out_specs=out_specs, check_vma=False
    )
```

```python
import functools

import jax
import jax.numpy as jnp
from jax import lax
from jax.experimental import pallas as pl
from jax.experimental.pallas import tpu as pltpu
from jax.sharding import PartitionSpec as P

MESH = pl.DeviceIdType.MESH
F32 = jnp.float32
BF16 = jnp.bfloat16
I32 = jnp.int32
SIDE = 4
CHIPS = SIDE**3
CHUNKS = 8
AHEAD = 5
CUT = (0, 24, 48, 64)
FAR = SIDE // 2


def destinations():
    near = [1, 3, 0]
    out = []
    for far in ((1, 1, 1), (1, 1, 0), (1, 0, 1), (0, 1, 1), (1, 0, 0), (0, 1, 0), (0, 0, 1), (0, 0, 0)):
        dims = [[FAR] if f else near for f in far]
        out += [(dx, dy, dz) for dz in dims[2] for dy in dims[1] for dx in dims[0]]
    return out


ORDER = destinations()
SLOT = {d: t for t, d in enumerate(ORDER)}


def others(d, p):
    return tuple(v for q, v in enumerate(d) if q != p)


def along(p, v, o):
    return o[:p] + (v,) + o[p:]


def plane_order():
    near = [1, 3, 0]
    out = [(FAR, FAR)] + [(FAR, b) for b in near] + [(a, FAR) for a in near]
    return out + [(a, b) for b in near for a in near]


PLANE = plane_order()
PLACE = {o: g for g, o in enumerate(PLANE)}
TEAM = [0] * 7 + [1] * 3 + [2] * 3 + [3] * 3
TEAMS = 4


def joined(o):
    return 1 if sum(o) % 2 == 0 else SIDE - 1


def kernel(
    dims,
    index_hbm,
    length_hbm,
    table_hbm,
    dense_hbm,
    wd_hbm,
    bias_hbm,
    sums_ref,
    start_ref,
    index_ref,
    length_ref,
    dense_ref,
    bias_ref,
    table,
    wd,
    outbox,
    inbox,
    ids_own,
    ids_mate,
    mate_out,
    own_rows,
    mate_rows,
    a_out,
    a_in,
    b_out,
    b_in,
    input_sem,
    table_sem,
    box_send,
    box_recv,
    fwd_send,
    fwd_recv,
    own_sem,
    rows_send,
    rows_recv,
    a_send,
    far_recv,
    near_recv,
    b_send,
    b_recv,
):
    local_rows, nt, slots_bag, cap = dims
    n = 2 * CHIPS
    samples, lanes = index_ref.shape
    bags = samples * nt
    total_rows = nt * local_rows
    r = lax.axis_index("rows")
    c = lax.axis_index("cols")
    x, z, y, k = r // SIDE, r % SIDE, c // 2, c % 2

    def step_by(at, d):
        return (at + d) % SIDE

    def device(xx, yy, zz, kk):
        return {"rows": xx * SIDE + zz, "cols": yy * 2 + kk}

    offsets = sorted(ORDER, key=lambda o: -sum(min(d, SIDE - d) for d in o))

    def shifted(d, kk):
        return device(step_by(x, d[0]), step_by(y, d[1]), step_by(z, d[2]), kk)

    inputs = [
        pltpu.make_async_copy(source, target, input_sem.at[i])
        for i, (source, target) in enumerate(
            (
                (index_hbm, index_ref),
                (length_hbm, length_ref),
                (wd_hbm, wd),
                (dense_hbm, dense_ref),
                (bias_hbm, bias_ref),
            )
        )
    ]
    for copy in inputs[:2]:
        copy.start()

    mate = device(x, y, z, 1 - k)

    barrier = pltpu.get_barrier_semaphore()
    for d in offsets:
        pl.semaphore_signal(barrier, inc=1, device_id=shifted(d, 1 - k), device_id_type=MESH)
        if any(d):
            pl.semaphore_signal(barrier, inc=1, device_id=shifted(d, k), device_id_type=MESH)

    inputs[0].wait()
    inputs[1].wait()
    for copy in inputs[2:]:
        copy.start()
    part = total_rows // CHUNKS
    for i in range(CHUNKS):
        pltpu.make_async_copy(
            table_hbm.at[pl.ds(i * part, part)], table.at[pl.ds(i * part, part)], table_sem
        ).start()

    idx = index_ref[...]
    lane = lax.broadcasted_iota(I32, (samples, lanes), 1)
    table_of = lane // slots_bag
    spread = jnp.where(
        lax.broadcasted_iota(I32, (nt, lanes), 1) // slots_bag == lax.broadcasted_iota(I32, (nt, lanes), 0),
        1.0,
        0.0,
    )
    length = lax.dot_general(
        length_ref[...].astype(F32).astype(BF16),
        spread.astype(BF16),
        (((0,), (0,)), ((), ())),
        preferred_element_type=F32,
    ).astype(I32)
    live = lane - table_of * slots_bag < length
    owner = idx // local_rows
    row = table_of * local_rows + idx - owner * local_rows
    bag = table_of * samples + lax.broadcasted_iota(I32, (samples, lanes), 0)
    owner = jnp.where(live, (owner % 2) * CHIPS + owner // 2, -1)
    pieces = []
    shift = 0
    while shift == 0 or (total_rows - 1) >> shift:
        pieces.append((row // (1 << shift)) % 256)
        shift += 8
    n_row = len(pieces)
    pieces.append(bag + 1)
    pieces = [v.astype(F32) for v in pieces]
    dev_iota = lax.broadcasted_iota(I32, (n, lanes), 0)
    before = (
        lax.broadcasted_iota(I32, (lanes, lanes), 0) < lax.broadcasted_iota(I32, (lanes, lanes), 1)
    )
    before = jnp.where(before, 1.0, 0.0).astype(BF16)
    hots = [
        jnp.where(owner[b : b + 1, :] == dev_iota, 1.0, 0.0).astype(F32) for b in range(samples)
    ]
    prefix = jnp.dot(
        jnp.concatenate([h.astype(BF16) for h in hots], axis=0), before, preferred_element_type=F32
    )
    base = jnp.zeros((n, 1), F32)
    box = jnp.zeros((len(pieces) * n, cap), F32)
    cap_iota = lax.broadcasted_iota(I32, (cap, lanes), 0)
    for b in range(samples):
        hot = hots[b]
        rank = jnp.sum(hot * (prefix[b * n : (b + 1) * n, :] + base), axis=0, keepdims=True)
        base = base + jnp.sum(hot, axis=1, keepdims=True)
        spot = jnp.where(rank.astype(I32) == cap_iota, 1.0, 0.0).astype(BF16)
        coded = jnp.concatenate([hot * v[b : b + 1, :] for v in pieces], axis=0).astype(BF16)
        box = box + lax.dot_general(
            coded, spot, (((1,), (1,)), ((), ())), preferred_element_type=F32
        )
    box_row = jnp.zeros((n, cap), I32)
    for i in range(n_row):
        box_row = box_row + box[i * n : (i + 1) * n, :].astype(I32) * (1 << (8 * i))
    box_bag = box[n_row * n :, :].astype(I32) - 1
    flip = jnp.full((CHIPS, cap), k, I32) == 1
    halves = []
    for both in (box_bag, box_row):
        halves.append(jnp.where(flip, both[CHIPS:], both[:CHIPS]))
        halves.append(jnp.where(flip, both[:CHIPS], both[CHIPS:]))
    boxes = jnp.concatenate(halves, axis=1) & (total_rows - 1)
    for d in range(CHIPS):
        outbox[d] = boxes[d : d + 1, :]

    def chip(xx, yy, zz):
        return (xx * SIDE + zz) * SIDE + yy

    inbox[SLOT[(0, 0, 0)]] = outbox[chip(x, y, z)]

    pl.semaphore_wait(barrier, n - 1)

    for d in offsets:
        back = tuple((SIDE - v) % SIDE for v in d)
        source = outbox.at[chip(step_by(x, back[0]), step_by(y, back[1]), step_by(z, back[2]))]
        pltpu.make_async_remote_copy(
            src_ref=source,
            dst_ref=ids_mate.at[SLOT[d]],
            send_sem=fwd_send,
            recv_sem=fwd_recv,
            device_id=shifted(back, 1 - k),
            device_id_type=MESH,
        ).start()
        if any(d):
            pltpu.make_async_remote_copy(
                src_ref=source,
                dst_ref=inbox.at[SLOT[d]],
                send_sem=box_send,
                recv_sem=box_recv,
                device_id=shifted(back, k),
                device_id_type=MESH,
            ).start()

    for copy in inputs[2:]:
        copy.wait()
    start_ref[...] = (
        jnp.dot(
            dense_ref[...], wd[...], precision=lax.Precision.HIGHEST, preferred_element_type=F32
        )
        + bias_ref[...]
    )

    rest = pl.ds(0, CHIPS - 1)
    boxes_moved = pltpu.make_async_remote_copy(
        src_ref=outbox.at[rest],
        dst_ref=inbox.at[rest],
        send_sem=box_send,
        recv_sem=box_recv,
        device_id=mate,
        device_id_type=MESH,
    )
    mates_moved = pltpu.make_async_remote_copy(
        src_ref=outbox,
        dst_ref=ids_mate,
        send_sem=fwd_send,
        recv_sem=fwd_recv,
        device_id=mate,
        device_id_type=MESH,
    )
    quarter = CHIPS // SIDE

    def own_copy(q):
        some = pl.ds(q * quarter, quarter)
        return pltpu.make_async_copy(inbox.at[some], ids_own.at[some], own_sem.at[q])

    boxes_moved.wait_recv()
    for q in range(SIDE):
        own_copy(q).start()
    mates_moved.wait_recv()
    pltpu.make_async_copy(table_hbm, table, table_sem).wait()

    def rows_copy(s):
        some = pl.ds(s * SIDE, SIDE)
        return pltpu.make_async_remote_copy(
            src_ref=mate_out.at[some],
            dst_ref=mate_rows.at[some],
            send_sem=rows_send,
            recv_sem=rows_recv.at[s],
            device_id=mate,
            device_id_type=MESH,
        )

    def fetch_mate(s):
        for u in range(SIDE):
            t = s * SIDE + u
            for i in range(cap):
                mate_out[t, i : i + 1, :] = table[pl.ds(ids_mate[t, 0, 3 * cap + i], 1), :]
        rows_copy(s).start()

    def fetch_own(s):
        for u in range(SIDE):
            t = s * SIDE + u
            for i in range(cap):
                own_rows[u, i : i + 1, :] = table[pl.ds(ids_own[t, 0, 2 * cap + i], 1), :]

    for s in range(AHEAD):
        fetch_mate(s)
    for q in range(SIDE):
        own_copy(q).wait()
    fetch_own(0)

    bag_iota = lax.broadcasted_iota(I32, (bags, 2 * cap), 0)

    def rows_of(p):
        return pl.ds(CUT[p], CUT[p + 1] - CUT[p])

    def a_copy(t, p, shift, recv):
        return pltpu.make_async_remote_copy(
            src_ref=a_out.at[t, rows_of(p)],
            dst_ref=a_in.at[t, rows_of(p)],
            send_sem=a_send,
            recv_sem=recv,
            device_id=shifted(along(p, shift, (0, 0)), k),
            device_id_type=MESH,
        )

    def b_copy(g, p):
        return pltpu.make_async_remote_copy(
            src_ref=b_out.at[g, rows_of(p)],
            dst_ref=b_in.at[g, rows_of(p)],
            send_sem=b_send,
            recv_sem=b_recv,
            device_id=shifted(along(p, 0, PLANE[g]), k),
            device_id_type=MESH,
        )

    def arrived(count, p, sem):
        pltpu.make_async_remote_copy(
            src_ref=a_in.at[pl.ds(0, count), rows_of(p)],
            dst_ref=a_in.at[pl.ds(0, count), rows_of(p)],
            send_sem=a_send,
            recv_sem=sem,
            device_id=mate,
            device_id_type=MESH,
        ).wait_recv()

    groups = CHIPS // SIDE

    def pool(s):
        rows_copy(s).wait_recv()
        slots = range(s * SIDE, (s + 1) * SIDE)
        for t in slots:
            found = jnp.concatenate([own_rows[t % SIDE], mate_rows[t]], axis=0)
            high = found.astype(BF16)
            low = (found - high.astype(F32)).astype(BF16)
            select = jnp.where(inbox[t, 0:1, 0 : 2 * cap] == bag_iota, 1.0, 0.0).astype(BF16)
            value = jnp.dot(select, high, preferred_element_type=F32) + jnp.dot(
                select, low, preferred_element_type=F32
            )
            a_out[t] = value
            for p in range(3):
                if ORDER[t][p] == 0:
                    a_in[t, CUT[p] : CUT[p + 1], :] = value[CUT[p] : CUT[p + 1]]
        if s + 1 < groups:
            fetch_own(s + 1)
        if s + AHEAD < groups:
            fetch_mate(s + AHEAD)
        for t in slots:
            for p in range(3):
                o, v = others(ORDER[t], p), ORDER[t][p]
                team = TEAM[PLACE[o]]
                if v == FAR:
                    a_copy(t, p, joined(o), far_recv.at[p, team]).start()
                elif v and v != joined(o):
                    a_copy(t, p, v, near_recv.at[p, team]).start()

    for s in range(groups):
        pool(s)
    for team in range(TEAMS):
        planes = [o for o in PLANE if TEAM[PLACE[o]] == team]
        for p in range(3):
            lo, hi = CUT[p], CUT[p + 1]
            arrived(len(planes), p, far_recv.at[p, team])
            for o in planes:
                t, far = SLOT[along(p, joined(o), o)], SLOT[along(p, FAR, o)]
                a_out[t, lo:hi, :] = a_out[t, lo:hi, :] + a_in[far, lo:hi, :]
                a_copy(t, p, joined(o), near_recv.at[p, team]).start()
    for team in range(TEAMS):
        planes = [o for o in PLANE if TEAM[PLACE[o]] == team]
        for p in range(3):
            lo, hi = CUT[p], CUT[p + 1]
            arrived(2 * len(planes), p, near_recv.at[p, team])
            for o in planes:
                g = PLACE[o]
                total = a_in[SLOT[along(p, 0, o)], lo:hi, :]
                for v in (1, SIDE - 1):
                    total = total + a_in[SLOT[along(p, v, o)], lo:hi, :]
                if any(o):
                    b_out[g, lo:hi, :] = total
                    b_copy(g, p).start()
                else:
                    b_in[g, lo:hi, :] = total

    some = pl.ds(0, groups - 1)
    b_moved = pltpu.make_async_remote_copy(
        src_ref=b_out.at[some],
        dst_ref=b_in.at[some],
        send_sem=b_send,
        recv_sem=b_recv,
        device_id=mate,
        device_id_type=MESH,
    )
    b_moved.wait_recv()
    pooled = b_in[0]
    for g in range(1, groups):
        pooled = pooled + b_in[g]

    sums_ref[...] = pooled

    boxes_moved.wait_send()
    mates_moved.wait_send()
    pltpu.make_async_remote_copy(
        src_ref=mate_out,
        dst_ref=mate_out,
        send_sem=rows_send,
        recv_sem=b_recv,
        device_id=mate,
        device_id_type=MESH,
    ).wait_send()
    some = pl.ds(0, CHIPS - groups)
    pltpu.make_async_remote_copy(
        src_ref=a_out.at[some],
        dst_ref=a_in.at[some],
        send_sem=a_send,
        recv_sem=b_recv,
        device_id=mate,
        device_id_type=MESH,
    ).wait_send()
    b_moved.wait_send()


def interact(sums_ref, start_ref, dense_ref, wp_ref, pooled_ref, hidden_ref):
    samples, nt = pooled_ref.shape[0], pooled_ref.shape[1]
    pooled = sums_ref[...]
    feats = [dense_ref[...]]
    for t in range(nt):
        feats.append(pooled[t * samples : (t + 1) * samples, :])
        pooled_ref[:, t, :] = feats[-1]
    total = start_ref[...]
    pair = 0
    for one in range(nt + 1):
        for two in range(one + 1, nt + 1):
            dots = jnp.sum(feats[one] * feats[two], axis=-1, keepdims=True)
            total = total + dots * wp_ref[pair : pair + 1, :]
            pair += 1
    hidden_ref[...] = jnp.maximum(total, 0.0)


def shards(bag_index, bag_length, emb_tables, dense_feats, w_dense, w_pair, top_bias):
    samples, lanes = bag_index.shape
    nt, local_rows, width = emb_tables.shape
    cap = 2 * samples * lanes // (2 * CHIPS)
    bags = samples * nt
    units = w_dense.shape[1]
    groups = CHIPS // SIDE
    dims = (local_rows, nt, lanes // nt, cap)
    vmem = pl.BlockSpec(memory_space=pltpu.VMEM)
    anyw = pl.BlockSpec(memory_space=pltpu.HBM)
    dma = pltpu.SemaphoreType.DMA
    sums, start = pl.pallas_call(
        functools.partial(kernel, dims),
        out_shape=(
            jax.ShapeDtypeStruct((bags, width), F32),
            jax.ShapeDtypeStruct((samples, units), F32),
        ),
        in_specs=[anyw] * 6,
        out_specs=(vmem, vmem),
        scratch_shapes=[
            pltpu.VMEM((samples, lanes), I32),
            pltpu.VMEM((nt, samples), I32),
            pltpu.VMEM((samples, width), F32),
            pltpu.VMEM((1, units), F32),
            pltpu.VMEM((nt * local_rows, width), F32),
            pltpu.VMEM(w_dense.shape, F32),
            pltpu.VMEM((CHIPS, 1, 4 * cap), I32),
            pltpu.VMEM((CHIPS, 1, 4 * cap), I32),
            pltpu.SMEM((CHIPS, 1, 4 * cap), I32),
            pltpu.SMEM((CHIPS, 1, 4 * cap), I32),
            pltpu.VMEM((CHIPS, cap, width), F32),
            pltpu.VMEM((SIDE, cap, width), F32),
            pltpu.VMEM((CHIPS, cap, width), F32),
            pltpu.VMEM((CHIPS, bags, width), F32),
            pltpu.VMEM((CHIPS, bags, width), F32),
            pltpu.VMEM((groups, bags, width), F32),
            pltpu.VMEM((groups, bags, width), F32),
            dma((5,)),
            dma,
            dma,
            dma,
            dma,
            dma,
            dma((SIDE,)),
            dma,
            dma((groups,)),
            dma,
            dma((3, TEAMS)),
            dma((3, TEAMS)),
            dma,
            dma,
        ],
        compiler_params=pltpu.CompilerParams(
            collective_id=0, has_side_effects=True, vmem_limit_bytes=40 * 1024 * 1024
        ),
    )(
        *(
            pltpu.with_memory_space_constraint(v, pltpu.HBM)
            for v in (
                bag_index,
                bag_length.T,
                emb_tables.reshape(nt * local_rows, width),
                dense_feats,
                w_dense,
                top_bias.reshape(1, units),
            )
        )
    )
    return pl.pallas_call(
        interact,
        out_shape=(
            jax.ShapeDtypeStruct((samples, nt, width), F32),
            jax.ShapeDtypeStruct((samples, units), F32),
        ),
        in_specs=[vmem] * 4,
        out_specs=(vmem, vmem),
        compiler_params=pltpu.CompilerParams(vmem_limit_bytes=8 * 1024 * 1024),
    )(sums, start, dense_feats, w_pair)


def solution(mesh):
    in_specs = (
        P(("rows", "cols"), None),
        P(("rows", "cols"), None),
        P(None, ("rows", "cols"), None),
        P(("rows", "cols"), None),
        P(),
        P(),
        P(),
    )
    out_specs = (P(("rows", "cols"), None, None), P(("rows", "cols"), None))
    return jax.shard_map(
        shards, mesh=mesh, in_specs=in_specs, out_specs=out_specs, check_vma=False
    )
```

```python
import functools

import jax
import jax.numpy as jnp
from jax import lax
from jax.experimental import pallas as pl
from jax.experimental.pallas import tpu as pltpu
from jax.sharding import PartitionSpec as P

MESH = pl.DeviceIdType.MESH
F32 = jnp.float32
BF16 = jnp.bfloat16
I32 = jnp.int32
SIDE = 4
CHIPS = SIDE**3
CHUNKS = 8
AHEAD = 5
CUT = (0, 24, 48, 64)
FAR = SIDE // 2


def destinations():
    near = [1, 3, 0]
    out = []
    for far in ((1, 1, 1), (1, 1, 0), (1, 0, 1), (0, 1, 1), (1, 0, 0), (0, 1, 0), (0, 0, 1), (0, 0, 0)):
        dims = [[FAR] if f else near for f in far]
        out += [(dx, dy, dz) for dz in dims[2] for dy in dims[1] for dx in dims[0]]
    return out


ORDER = destinations()
SLOT = {d: t for t, d in enumerate(ORDER)}


def others(d, p):
    return tuple(v for q, v in enumerate(d) if q != p)


def along(p, v, o):
    return o[:p] + (v,) + o[p:]


def plane_order():
    near = [1, 3, 0]
    out = [(FAR, FAR)] + [(FAR, b) for b in near] + [(a, FAR) for a in near]
    return out + [(a, b) for b in near for a in near]


PLANE = plane_order()
PLACE = {o: g for g, o in enumerate(PLANE)}
TEAM = [0] * 4 + [1] * 3 + [2] * 3 + [3] * 3 + [4] * 3
TEAMS = 5
EARLY = {13: 0, 15: 1}


def joined(o):
    return 1 if sum(o) % 2 == 0 else SIDE - 1


def kernel(
    dims,
    index_hbm,
    length_hbm,
    table_hbm,
    dense_hbm,
    wd_hbm,
    bias_hbm,
    sums_ref,
    start_ref,
    index_ref,
    length_ref,
    dense_ref,
    bias_ref,
    table,
    wd,
    outbox,
    inbox,
    ids_own,
    ids_mate,
    mate_out,
    own_rows,
    mate_rows,
    a_out,
    a_in,
    b_out,
    b_in,
    input_sem,
    table_sem,
    box_send,
    box_recv,
    fwd_send,
    fwd_recv,
    own_sem,
    rows_send,
    rows_recv,
    a_send,
    far_recv,
    near_recv,
    b_send,
    b_recv,
):
    local_rows, nt, slots_bag, cap = dims
    n = 2 * CHIPS
    samples, lanes = index_ref.shape
    bags = samples * nt
    total_rows = nt * local_rows
    r = lax.axis_index("rows")
    c = lax.axis_index("cols")
    x, z, y, k = r // SIDE, r % SIDE, c // 2, c % 2

    def step_by(at, d):
        return (at + d) % SIDE

    def device(xx, yy, zz, kk):
        return {"rows": xx * SIDE + zz, "cols": yy * 2 + kk}

    offsets = sorted(ORDER, key=lambda o: -sum(min(d, SIDE - d) for d in o))

    def shifted(d, kk):
        return device(step_by(x, d[0]), step_by(y, d[1]), step_by(z, d[2]), kk)

    inputs = [
        pltpu.make_async_copy(source, target, input_sem.at[i])
        for i, (source, target) in enumerate(
            (
                (index_hbm, index_ref),
                (length_hbm, length_ref),
                (wd_hbm, wd),
                (dense_hbm, dense_ref),
                (bias_hbm, bias_ref),
            )
        )
    ]
    for copy in inputs[:2]:
        copy.start()

    mate = device(x, y, z, 1 - k)

    barrier = pltpu.get_barrier_semaphore()
    for d in offsets:
        pl.semaphore_signal(barrier, inc=1, device_id=shifted(d, 1 - k), device_id_type=MESH)
        if any(d):
            pl.semaphore_signal(barrier, inc=1, device_id=shifted(d, k), device_id_type=MESH)

    inputs[0].wait()
    inputs[1].wait()
    for copy in inputs[2:]:
        copy.start()
    part = total_rows // CHUNKS
    for i in range(CHUNKS):
        pltpu.make_async_copy(
            table_hbm.at[pl.ds(i * part, part)], table.at[pl.ds(i * part, part)], table_sem
        ).start()

    idx = index_ref[...]
    lane = lax.broadcasted_iota(I32, (samples, lanes), 1)
    table_of = lane // slots_bag
    spread = jnp.where(
        lax.broadcasted_iota(I32, (nt, lanes), 1) // slots_bag == lax.broadcasted_iota(I32, (nt, lanes), 0),
        1.0,
        0.0,
    )
    length = lax.dot_general(
        length_ref[...].astype(F32).astype(BF16),
        spread.astype(BF16),
        (((0,), (0,)), ((), ())),
        preferred_element_type=F32,
    ).astype(I32)
    live = lane - table_of * slots_bag < length
    owner = idx // local_rows
    row = table_of * local_rows + idx - owner * local_rows
    bag = table_of * samples + lax.broadcasted_iota(I32, (samples, lanes), 0)
    owner = jnp.where(live, (owner % 2) * CHIPS + owner // 2, -1)
    pieces = []
    shift = 0
    while shift == 0 or (total_rows - 1) >> shift:
        pieces.append((row // (1 << shift)) % 256)
        shift += 8
    n_row = len(pieces)
    pieces.append(bag + 1)
    pieces = [v.astype(F32) for v in pieces]
    dev_iota = lax.broadcasted_iota(I32, (n, lanes), 0)
    before = (
        lax.broadcasted_iota(I32, (lanes, lanes), 0) < lax.broadcasted_iota(I32, (lanes, lanes), 1)
    )
    before = jnp.where(before, 1.0, 0.0).astype(BF16)
    hots = [
        jnp.where(owner[b : b + 1, :] == dev_iota, 1.0, 0.0).astype(F32) for b in range(samples)
    ]
    prefix = jnp.dot(
        jnp.concatenate([h.astype(BF16) for h in hots], axis=0), before, preferred_element_type=F32
    )
    base = jnp.zeros((n, 1), F32)
    box = jnp.zeros((len(pieces) * n, cap), F32)
    cap_iota = lax.broadcasted_iota(I32, (cap, lanes), 0)
    for b in range(samples):
        hot = hots[b]
        rank = jnp.sum(hot * (prefix[b * n : (b + 1) * n, :] + base), axis=0, keepdims=True)
        base = base + jnp.sum(hot, axis=1, keepdims=True)
        spot = jnp.where(rank.astype(I32) == cap_iota, 1.0, 0.0).astype(BF16)
        coded = jnp.concatenate([hot * v[b : b + 1, :] for v in pieces], axis=0).astype(BF16)
        box = box + lax.dot_general(
            coded, spot, (((1,), (1,)), ((), ())), preferred_element_type=F32
        )
    box_row = jnp.zeros((n, cap), I32)
    for i in range(n_row):
        box_row = box_row + box[i * n : (i + 1) * n, :].astype(I32) * (1 << (8 * i))
    box_bag = box[n_row * n :, :].astype(I32) - 1
    flip = jnp.full((CHIPS, cap), k, I32) == 1
    halves = []
    for both in (box_bag, box_row):
        halves.append(jnp.where(flip, both[CHIPS:], both[:CHIPS]))
        halves.append(jnp.where(flip, both[:CHIPS], both[CHIPS:]))
    boxes = jnp.concatenate(halves, axis=1) & (total_rows - 1)
    for d in range(CHIPS):
        outbox[d] = boxes[d : d + 1, :]

    def chip(xx, yy, zz):
        return (xx * SIDE + zz) * SIDE + yy

    inbox[SLOT[(0, 0, 0)]] = outbox[chip(x, y, z)]

    pl.semaphore_wait(barrier, n - 1)

    for d in offsets:
        back = tuple((SIDE - v) % SIDE for v in d)
        source = outbox.at[chip(step_by(x, back[0]), step_by(y, back[1]), step_by(z, back[2]))]
        pltpu.make_async_remote_copy(
            src_ref=source,
            dst_ref=ids_mate.at[SLOT[d]],
            send_sem=fwd_send,
            recv_sem=fwd_recv,
            device_id=shifted(back, 1 - k),
            device_id_type=MESH,
        ).start()
        if any(d):
            pltpu.make_async_remote_copy(
                src_ref=source,
                dst_ref=inbox.at[SLOT[d]],
                send_sem=box_send,
                recv_sem=box_recv,
                device_id=shifted(back, k),
                device_id_type=MESH,
            ).start()

    for copy in inputs[2:]:
        copy.wait()
    start_ref[...] = (
        jnp.dot(
            dense_ref[...], wd[...], precision=lax.Precision.HIGHEST, preferred_element_type=F32
        )
        + bias_ref[...]
    )

    rest = pl.ds(0, CHIPS - 1)
    boxes_moved = pltpu.make_async_remote_copy(
        src_ref=outbox.at[rest],
        dst_ref=inbox.at[rest],
        send_sem=box_send,
        recv_sem=box_recv,
        device_id=mate,
        device_id_type=MESH,
    )
    mates_moved = pltpu.make_async_remote_copy(
        src_ref=outbox,
        dst_ref=ids_mate,
        send_sem=fwd_send,
        recv_sem=fwd_recv,
        device_id=mate,
        device_id_type=MESH,
    )

    own_copy = pltpu.make_async_copy(inbox, ids_own, own_sem)
    boxes_moved.wait_recv()
    own_copy.start()
    mates_moved.wait_recv()
    pltpu.make_async_copy(table_hbm, table, table_sem).wait()

    def rows_copy(s):
        some = pl.ds(s * SIDE, SIDE)
        return pltpu.make_async_remote_copy(
            src_ref=mate_out.at[some],
            dst_ref=mate_rows.at[some],
            send_sem=rows_send,
            recv_sem=rows_recv.at[s],
            device_id=mate,
            device_id_type=MESH,
        )

    def fetch_mate(s):
        for u in range(SIDE):
            t = s * SIDE + u
            for i in range(cap):
                mate_out[t, i : i + 1, :] = table[pl.ds(ids_mate[t, 0, 3 * cap + i], 1), :]
        rows_copy(s).start()

    def fetch_own(s):
        for u in range(SIDE):
            t = s * SIDE + u
            for i in range(cap):
                own_rows[u, i : i + 1, :] = table[pl.ds(ids_own[t, 0, 2 * cap + i], 1), :]

    def fetch_ahead(s, carry):
        fetch_mate(s)
        return carry

    lax.fori_loop(0, AHEAD, fetch_ahead, 0)
    own_copy.wait()
    fetch_own(0)

    bag_iota = lax.broadcasted_iota(I32, (bags, 2 * cap), 0)

    def rows_of(p):
        return pl.ds(CUT[p], CUT[p + 1] - CUT[p])

    def a_copy(t, p, shift, recv):
        return pltpu.make_async_remote_copy(
            src_ref=a_out.at[t, rows_of(p)],
            dst_ref=a_in.at[t, rows_of(p)],
            send_sem=a_send,
            recv_sem=recv,
            device_id=shifted(along(p, shift, (0, 0)), k),
            device_id_type=MESH,
        )

    def b_copy(g, p):
        return pltpu.make_async_remote_copy(
            src_ref=b_out.at[g, rows_of(p)],
            dst_ref=b_in.at[g, rows_of(p)],
            send_sem=b_send,
            recv_sem=b_recv,
            device_id=shifted(along(p, 0, PLANE[g]), k),
            device_id_type=MESH,
        )

    def arrived(count, p, sem):
        pltpu.make_async_remote_copy(
            src_ref=a_in.at[pl.ds(0, count), rows_of(p)],
            dst_ref=a_in.at[pl.ds(0, count), rows_of(p)],
            send_sem=a_send,
            recv_sem=sem,
            device_id=mate,
            device_id_type=MESH,
        ).wait_recv()

    groups = CHIPS // SIDE

    def pool(s):
        rows_copy(s).wait_recv()
        slots = range(s * SIDE, (s + 1) * SIDE)
        for t in slots:
            found = jnp.concatenate([own_rows[t % SIDE], mate_rows[t]], axis=0)
            high = found.astype(BF16)
            low = (found - high.astype(F32)).astype(BF16)
            select = jnp.where(inbox[t, 0:1, 0 : 2 * cap] == bag_iota, 1.0, 0.0).astype(BF16)
            value = jnp.dot(select, high, preferred_element_type=F32) + jnp.dot(
                select, low, preferred_element_type=F32
            )
            a_out[t] = value
            for p in range(3):
                if ORDER[t][p] == 0:
                    a_in[t, CUT[p] : CUT[p + 1], :] = value[CUT[p] : CUT[p + 1]]
        if s + 1 < groups:
            fetch_own(s + 1)
        if s + AHEAD < groups:
            fetch_mate(s + AHEAD)
        for t in slots:
            for p in range(3):
                o, v = others(ORDER[t], p), ORDER[t][p]
                team = TEAM[PLACE[o]]
                if v == FAR:
                    a_copy(t, p, joined(o), far_recv.at[p, team]).start()
                elif v and v != joined(o):
                    a_copy(t, p, v, near_recv.at[p, team]).start()

    def relay(team):
        planes = [o for o in PLANE if TEAM[PLACE[o]] == team]
        for p in range(3):
            lo, hi = CUT[p], CUT[p + 1]
            arrived(len(planes), p, far_recv.at[p, team])
            for o in planes:
                t, far = SLOT[along(p, joined(o), o)], SLOT[along(p, FAR, o)]
                a_out[t, lo:hi, :] = a_out[t, lo:hi, :] + a_in[far, lo:hi, :]
                a_copy(t, p, joined(o), near_recv.at[p, team]).start()

    for s in range(groups):
        pool(s)
        if s in EARLY:
            relay(EARLY[s])
    for team in range(TEAMS):
        if team not in EARLY.values():
            relay(team)
    for team in range(TEAMS):
        planes = [o for o in PLANE if TEAM[PLACE[o]] == team]
        for p in range(3):
            lo, hi = CUT[p], CUT[p + 1]
            arrived(2 * len(planes), p, near_recv.at[p, team])
            for o in planes:
                g = PLACE[o]
                total = a_in[SLOT[along(p, 0, o)], lo:hi, :]
                for v in (1, SIDE - 1):
                    total = total + a_in[SLOT[along(p, v, o)], lo:hi, :]
                if any(o):
                    b_out[g, lo:hi, :] = total
                    b_copy(g, p).start()
                else:
                    b_in[g, lo:hi, :] = total

    some = pl.ds(0, groups - 1)
    b_moved = pltpu.make_async_remote_copy(
        src_ref=b_out.at[some],
        dst_ref=b_in.at[some],
        send_sem=b_send,
        recv_sem=b_recv,
        device_id=mate,
        device_id_type=MESH,
    )
    b_moved.wait_recv()
    pooled = b_in[0]
    for g in range(1, groups):
        pooled = pooled + b_in[g]

    sums_ref[...] = pooled

    boxes_moved.wait_send()
    mates_moved.wait_send()
    pltpu.make_async_remote_copy(
        src_ref=mate_out,
        dst_ref=mate_out,
        send_sem=rows_send,
        recv_sem=b_recv,
        device_id=mate,
        device_id_type=MESH,
    ).wait_send()
    some = pl.ds(0, CHIPS - groups)
    pltpu.make_async_remote_copy(
        src_ref=a_out.at[some],
        dst_ref=a_in.at[some],
        send_sem=a_send,
        recv_sem=b_recv,
        device_id=mate,
        device_id_type=MESH,
    ).wait_send()
    b_moved.wait_send()


def interact(sums_ref, start_ref, dense_ref, wp_ref, pooled_ref, hidden_ref):
    samples, nt = pooled_ref.shape[0], pooled_ref.shape[1]
    pooled = sums_ref[...]
    feats = [dense_ref[...]]
    for t in range(nt):
        feats.append(pooled[t * samples : (t + 1) * samples, :])
        pooled_ref[:, t, :] = feats[-1]
    total = start_ref[...]
    pair = 0
    for one in range(nt + 1):
        for two in range(one + 1, nt + 1):
            dots = jnp.sum(feats[one] * feats[two], axis=-1, keepdims=True)
            total = total + dots * wp_ref[pair : pair + 1, :]
            pair += 1
    hidden_ref[...] = jnp.maximum(total, 0.0)


def shards(bag_index, bag_length, emb_tables, dense_feats, w_dense, w_pair, top_bias):
    samples, lanes = bag_index.shape
    nt, local_rows, width = emb_tables.shape
    cap = 2 * samples * lanes // (2 * CHIPS)
    bags = samples * nt
    units = w_dense.shape[1]
    groups = CHIPS // SIDE
    dims = (local_rows, nt, lanes // nt, cap)
    vmem = pl.BlockSpec(memory_space=pltpu.VMEM)
    anyw = pl.BlockSpec(memory_space=pltpu.HBM)
    dma = pltpu.SemaphoreType.DMA
    sums, start = pl.pallas_call(
        functools.partial(kernel, dims),
        out_shape=(
            jax.ShapeDtypeStruct((bags, width), F32),
            jax.ShapeDtypeStruct((samples, units), F32),
        ),
        in_specs=[anyw] * 6,
        out_specs=(vmem, vmem),
        scratch_shapes=[
            pltpu.VMEM((samples, lanes), I32),
            pltpu.VMEM((nt, samples), I32),
            pltpu.VMEM((samples, width), F32),
            pltpu.VMEM((1, units), F32),
            pltpu.VMEM((nt * local_rows, width), F32),
            pltpu.VMEM(w_dense.shape, F32),
            pltpu.VMEM((CHIPS, 1, 4 * cap), I32),
            pltpu.VMEM((CHIPS, 1, 4 * cap), I32),
            pltpu.SMEM((CHIPS, 1, 4 * cap), I32),
            pltpu.SMEM((CHIPS, 1, 4 * cap), I32),
            pltpu.VMEM((CHIPS, cap, width), F32),
            pltpu.VMEM((SIDE, cap, width), F32),
            pltpu.VMEM((CHIPS, cap, width), F32),
            pltpu.VMEM((CHIPS, bags, width), F32),
            pltpu.VMEM((CHIPS, bags, width), F32),
            pltpu.VMEM((groups, bags, width), F32),
            pltpu.VMEM((groups, bags, width), F32),
            dma((5,)),
            dma,
            dma,
            dma,
            dma,
            dma,
            dma,
            dma,
            dma((groups,)),
            dma,
            dma((3, TEAMS)),
            dma((3, TEAMS)),
            dma,
            dma,
        ],
        compiler_params=pltpu.CompilerParams(
            collective_id=0, has_side_effects=True, vmem_limit_bytes=40 * 1024 * 1024
        ),
    )(
        *(
            pltpu.with_memory_space_constraint(v, pltpu.HBM)
            for v in (
                bag_index,
                bag_length.T,
                emb_tables.reshape(nt * local_rows, width),
                dense_feats,
                w_dense,
                top_bias.reshape(1, units),
            )
        )
    )
    return pl.pallas_call(
        interact,
        out_shape=(
            jax.ShapeDtypeStruct((samples, nt, width), F32),
            jax.ShapeDtypeStruct((samples, units), F32),
        ),
        in_specs=[vmem] * 4,
        out_specs=(vmem, vmem),
        compiler_params=pltpu.CompilerParams(vmem_limit_bytes=8 * 1024 * 1024),
    )(sums, start, dense_feats, w_pair)


def solution(mesh):
    in_specs = (
        P(("rows", "cols"), None),
        P(("rows", "cols"), None),
        P(None, ("rows", "cols"), None),
        P(("rows", "cols"), None),
        P(),
        P(),
        P(),
    )
    out_specs = (P(("rows", "cols"), None, None), P(("rows", "cols"), None))
    return jax.shard_map(
        shards, mesh=mesh, in_specs=in_specs, out_specs=out_specs, check_vma=False
    )
```

```python
import functools

import jax
import jax.numpy as jnp
from jax import lax
from jax.experimental import pallas as pl
from jax.experimental.pallas import tpu as pltpu
from jax.sharding import PartitionSpec as P

MESH = pl.DeviceIdType.MESH
F32 = jnp.float32
BF16 = jnp.bfloat16
I32 = jnp.int32
SIDE = 4
CHIPS = SIDE**3
CHUNKS = 8
AHEAD = 5
FIRST = (16, 24, 16, 24)
SECOND = (40, 40, 48, 40)
BAGS = 64
FAR = SIDE // 2


def destinations():
    near = [1, 3, 0]
    out = []
    for far in ((1, 1, 1), (1, 1, 0), (1, 0, 1), (0, 1, 1), (1, 0, 0), (0, 1, 0), (0, 0, 1), (0, 0, 0)):
        dims = [[FAR] if f else near for f in far]
        out += [(dx, dy, dz) for dz in dims[2] for dy in dims[1] for dx in dims[0]]
    return out


ORDER = destinations()
SLOT = {d: t for t, d in enumerate(ORDER)}


def others(d, p):
    return tuple(v for q, v in enumerate(d) if q != p)


def along(p, v, o):
    return o[:p] + (v,) + o[p:]


def plane_order():
    near = [1, 3, 0]
    out = [(FAR, FAR)] + [(FAR, b) for b in near] + [(a, FAR) for a in near]
    return out + [(a, b) for b in near for a in near]


PLANE = plane_order()
PLACE = {o: g for g, o in enumerate(PLANE)}
TEAM = [0] * 4 + [1] * 3 + [2] * 3 + [3] * 3 + [4] * 3
TEAMS = 5
EARLY = {13: 0, 15: 1}


def span(p, o):
    a, b = o
    return ((0, FIRST[b]), (FIRST[b], SECOND[a]), (SECOND[a], BAGS))[p]


def height(p, planes):
    return sum(span(p, o)[1] - span(p, o)[0] for o in planes)


def joined(o):
    return 1 if sum(o) % 2 == 0 else SIDE - 1


def kernel(
    dims,
    index_hbm,
    length_hbm,
    table_hbm,
    dense_hbm,
    wd_hbm,
    bias_hbm,
    sums_ref,
    start_ref,
    index_ref,
    length_ref,
    dense_ref,
    bias_ref,
    table,
    wd,
    outbox,
    inbox,
    ids_own,
    ids_mate,
    mate_out,
    own_rows,
    mate_rows,
    a_out,
    a_in,
    b_out,
    b_in,
    input_sem,
    table_sem,
    box_send,
    box_recv,
    fwd_send,
    fwd_recv,
    own_sem,
    rows_send,
    rows_recv,
    a_send,
    far_recv,
    near_recv,
    b_send,
    b_recv,
):
    local_rows, nt, slots_bag, cap = dims
    n = 2 * CHIPS
    samples, lanes = index_ref.shape
    bags = samples * nt
    total_rows = nt * local_rows
    r = lax.axis_index("rows")
    c = lax.axis_index("cols")
    x, z, y, k = r // SIDE, r % SIDE, c // 2, c % 2

    def step_by(at, d):
        return (at + d) % SIDE

    def device(xx, yy, zz, kk):
        return {"rows": xx * SIDE + zz, "cols": yy * 2 + kk}

    offsets = sorted(ORDER, key=lambda o: -sum(min(d, SIDE - d) for d in o))

    def shifted(d, kk):
        return device(step_by(x, d[0]), step_by(y, d[1]), step_by(z, d[2]), kk)

    inputs = [
        pltpu.make_async_copy(source, target, input_sem.at[i])
        for i, (source, target) in enumerate(
            (
                (index_hbm, index_ref),
                (length_hbm, length_ref),
                (wd_hbm, wd),
                (dense_hbm, dense_ref),
                (bias_hbm, bias_ref),
            )
        )
    ]
    for copy in inputs[:2]:
        copy.start()

    mate = device(x, y, z, 1 - k)

    barrier = pltpu.get_barrier_semaphore()
    for d in offsets:
        pl.semaphore_signal(barrier, inc=1, device_id=shifted(d, 1 - k), device_id_type=MESH)
        if any(d):
            pl.semaphore_signal(barrier, inc=1, device_id=shifted(d, k), device_id_type=MESH)

    inputs[0].wait()
    inputs[1].wait()
    for copy in inputs[2:]:
        copy.start()
    part = total_rows // CHUNKS
    for i in range(CHUNKS):
        pltpu.make_async_copy(
            table_hbm.at[pl.ds(i * part, part)], table.at[pl.ds(i * part, part)], table_sem
        ).start()

    idx = index_ref[...]
    lane = lax.broadcasted_iota(I32, (samples, lanes), 1)
    table_of = lane // slots_bag
    spread = jnp.where(
        lax.broadcasted_iota(I32, (nt, lanes), 1) // slots_bag == lax.broadcasted_iota(I32, (nt, lanes), 0),
        1.0,
        0.0,
    )
    length = lax.dot_general(
        length_ref[...].astype(F32).astype(BF16),
        spread.astype(BF16),
        (((0,), (0,)), ((), ())),
        preferred_element_type=F32,
    ).astype(I32)
    live = lane - table_of * slots_bag < length
    owner = idx // local_rows
    row = table_of * local_rows + idx - owner * local_rows
    bag = table_of * samples + lax.broadcasted_iota(I32, (samples, lanes), 0)
    owner = jnp.where(live, (owner % 2) * CHIPS + owner // 2, -1)
    pieces = []
    shift = 0
    while shift == 0 or (total_rows - 1) >> shift:
        pieces.append((row // (1 << shift)) % 256)
        shift += 8
    n_row = len(pieces)
    pieces.append(bag + 1)
    pieces = [v.astype(F32) for v in pieces]
    dev_iota = lax.broadcasted_iota(I32, (n, lanes), 0)
    before = (
        lax.broadcasted_iota(I32, (lanes, lanes), 0) < lax.broadcasted_iota(I32, (lanes, lanes), 1)
    )
    before = jnp.where(before, 1.0, 0.0).astype(BF16)
    hots = [
        jnp.where(owner[b : b + 1, :] == dev_iota, 1.0, 0.0).astype(F32) for b in range(samples)
    ]
    prefix = jnp.dot(
        jnp.concatenate([h.astype(BF16) for h in hots], axis=0), before, preferred_element_type=F32
    )
    base = jnp.zeros((n, 1), F32)
    box = jnp.zeros((len(pieces) * n, cap), F32)
    cap_iota = lax.broadcasted_iota(I32, (cap, lanes), 0)
    for b in range(samples):
        hot = hots[b]
        rank = jnp.sum(hot * (prefix[b * n : (b + 1) * n, :] + base), axis=0, keepdims=True)
        base = base + jnp.sum(hot, axis=1, keepdims=True)
        spot = jnp.where(rank.astype(I32) == cap_iota, 1.0, 0.0).astype(BF16)
        coded = jnp.concatenate([hot * v[b : b + 1, :] for v in pieces], axis=0).astype(BF16)
        box = box + lax.dot_general(
            coded, spot, (((1,), (1,)), ((), ())), preferred_element_type=F32
        )
    box_row = jnp.zeros((n, cap), I32)
    for i in range(n_row):
        box_row = box_row + box[i * n : (i + 1) * n, :].astype(I32) * (1 << (8 * i))
    box_bag = box[n_row * n :, :].astype(I32) - 1
    flip = jnp.full((CHIPS, cap), k, I32) == 1
    halves = []
    for both in (box_bag, box_row):
        halves.append(jnp.where(flip, both[CHIPS:], both[:CHIPS]))
        halves.append(jnp.where(flip, both[:CHIPS], both[CHIPS:]))
    boxes = jnp.concatenate(halves, axis=1) & (total_rows - 1)
    for d in range(CHIPS):
        outbox[d] = boxes[d : d + 1, :]

    def chip(xx, yy, zz):
        return (xx * SIDE + zz) * SIDE + yy

    inbox[SLOT[(0, 0, 0)]] = outbox[chip(x, y, z)]

    pl.semaphore_wait(barrier, n - 1)

    for d in offsets:
        back = tuple((SIDE - v) % SIDE for v in d)
        source = outbox.at[chip(step_by(x, back[0]), step_by(y, back[1]), step_by(z, back[2]))]
        pltpu.make_async_remote_copy(
            src_ref=source,
            dst_ref=ids_mate.at[SLOT[d]],
            send_sem=fwd_send,
            recv_sem=fwd_recv,
            device_id=shifted(back, 1 - k),
            device_id_type=MESH,
        ).start()
        if any(d):
            pltpu.make_async_remote_copy(
                src_ref=source,
                dst_ref=inbox.at[SLOT[d]],
                send_sem=box_send,
                recv_sem=box_recv,
                device_id=shifted(back, k),
                device_id_type=MESH,
            ).start()

    for copy in inputs[2:]:
        copy.wait()
    start_ref[...] = (
        jnp.dot(
            dense_ref[...], wd[...], precision=lax.Precision.HIGHEST, preferred_element_type=F32
        )
        + bias_ref[...]
    )

    rest = pl.ds(0, CHIPS - 1)
    boxes_moved = pltpu.make_async_remote_copy(
        src_ref=outbox.at[rest],
        dst_ref=inbox.at[rest],
        send_sem=box_send,
        recv_sem=box_recv,
        device_id=mate,
        device_id_type=MESH,
    )
    mates_moved = pltpu.make_async_remote_copy(
        src_ref=outbox,
        dst_ref=ids_mate,
        send_sem=fwd_send,
        recv_sem=fwd_recv,
        device_id=mate,
        device_id_type=MESH,
    )

    own_copy = pltpu.make_async_copy(inbox, ids_own, own_sem)
    boxes_moved.wait_recv()
    own_copy.start()
    mates_moved.wait_recv()
    pltpu.make_async_copy(table_hbm, table, table_sem).wait()

    def rows_copy(s):
        some = pl.ds(s * SIDE, SIDE)
        return pltpu.make_async_remote_copy(
            src_ref=mate_out.at[some],
            dst_ref=mate_rows.at[some],
            send_sem=rows_send,
            recv_sem=rows_recv.at[s],
            device_id=mate,
            device_id_type=MESH,
        )

    def fetch_mate(s):
        for u in range(SIDE):
            t = s * SIDE + u
            for i in range(cap):
                mate_out[t, i : i + 1, :] = table[pl.ds(ids_mate[t, 0, 3 * cap + i], 1), :]
        rows_copy(s).start()

    def fetch_own(s):
        for u in range(SIDE):
            t = s * SIDE + u
            for i in range(cap):
                own_rows[u, i : i + 1, :] = table[pl.ds(ids_own[t, 0, 2 * cap + i], 1), :]

    def fetch_ahead(s, carry):
        fetch_mate(s)
        return carry

    lax.fori_loop(0, AHEAD, fetch_ahead, 0)
    own_copy.wait()
    fetch_own(0)

    bag_iota = lax.broadcasted_iota(I32, (bags, 2 * cap), 0)

    def rows_of(p, o):
        lo, hi = span(p, o)
        return pl.ds(lo, hi - lo)

    def a_copy(t, p, shift, recv):
        rows = rows_of(p, others(ORDER[t], p))
        return pltpu.make_async_remote_copy(
            src_ref=a_out.at[t, rows],
            dst_ref=a_in.at[t, rows],
            send_sem=a_send,
            recv_sem=recv,
            device_id=shifted(along(p, shift, (0, 0)), k),
            device_id_type=MESH,
        )

    def b_copy(g, p):
        return pltpu.make_async_remote_copy(
            src_ref=b_out.at[g, rows_of(p, PLANE[g])],
            dst_ref=b_in.at[g, rows_of(p, PLANE[g])],
            send_sem=b_send,
            recv_sem=b_recv,
            device_id=shifted(along(p, 0, PLANE[g]), k),
            device_id_type=MESH,
        )

    def arrived(count, sem):
        tiles, some = pl.ds(0, count // 8), pl.ds(0, 8)
        pltpu.make_async_remote_copy(
            src_ref=a_in.at[tiles, some],
            dst_ref=a_in.at[tiles, some],
            send_sem=a_send,
            recv_sem=sem,
            device_id=mate,
            device_id_type=MESH,
        ).wait_recv()

    groups = CHIPS // SIDE

    def pool(s):
        rows_copy(s).wait_recv()
        slots = range(s * SIDE, (s + 1) * SIDE)
        for t in slots:
            found = jnp.concatenate([own_rows[t % SIDE], mate_rows[t]], axis=0)
            high = found.astype(BF16)
            low = (found - high.astype(F32)).astype(BF16)
            select = jnp.where(inbox[t, 0:1, 0 : 2 * cap] == bag_iota, 1.0, 0.0).astype(BF16)
            value = jnp.dot(select, high, preferred_element_type=F32) + jnp.dot(
                select, low, preferred_element_type=F32
            )
            a_out[t] = value
            for p in range(3):
                if ORDER[t][p] == 0:
                    lo, hi = span(p, others(ORDER[t], p))
                    a_in[t, lo:hi, :] = value[lo:hi]
        if s + 1 < groups:
            fetch_own(s + 1)
        if s + AHEAD < groups:
            fetch_mate(s + AHEAD)
        for t in slots:
            for p in range(3):
                o, v = others(ORDER[t], p), ORDER[t][p]
                team = TEAM[PLACE[o]]
                if v == FAR:
                    a_copy(t, p, joined(o), far_recv.at[p, team]).start()
                elif v and v != joined(o):
                    a_copy(t, p, v, near_recv.at[p, team]).start()

    def relay(team):
        planes = [o for o in PLANE if TEAM[PLACE[o]] == team]
        for p in range(3):
            arrived(height(p, planes), far_recv.at[p, team])
            for o in planes:
                lo, hi = span(p, o)
                t, far = SLOT[along(p, joined(o), o)], SLOT[along(p, FAR, o)]
                a_out[t, lo:hi, :] = a_out[t, lo:hi, :] + a_in[far, lo:hi, :]
                a_copy(t, p, joined(o), near_recv.at[p, team]).start()

    for s in range(groups):
        pool(s)
        if s in EARLY:
            relay(EARLY[s])
    for team in range(TEAMS):
        if team not in EARLY.values():
            relay(team)
    for team in range(TEAMS):
        planes = [o for o in PLANE if TEAM[PLACE[o]] == team]
        for p in range(3):
            arrived(2 * height(p, planes), near_recv.at[p, team])
            for o in planes:
                lo, hi = span(p, o)
                g = PLACE[o]
                total = a_in[SLOT[along(p, 0, o)], lo:hi, :]
                for v in (1, SIDE - 1):
                    total = total + a_in[SLOT[along(p, v, o)], lo:hi, :]
                if any(o):
                    b_out[g, lo:hi, :] = total
                    b_copy(g, p).start()
                else:
                    b_in[g, lo:hi, :] = total

    some = pl.ds(0, groups - 1)
    b_moved = pltpu.make_async_remote_copy(
        src_ref=b_out.at[some],
        dst_ref=b_in.at[some],
        send_sem=b_send,
        recv_sem=b_recv,
        device_id=mate,
        device_id_type=MESH,
    )
    b_moved.wait_recv()
    pooled = b_in[0]
    for g in range(1, groups):
        pooled = pooled + b_in[g]

    sums_ref[...] = pooled

    boxes_moved.wait_send()
    mates_moved.wait_send()
    pltpu.make_async_remote_copy(
        src_ref=mate_out,
        dst_ref=mate_out,
        send_sem=rows_send,
        recv_sem=b_recv,
        device_id=mate,
        device_id_type=MESH,
    ).wait_send()
    some = pl.ds(0, CHIPS - groups)
    pltpu.make_async_remote_copy(
        src_ref=a_out.at[some],
        dst_ref=a_in.at[some],
        send_sem=a_send,
        recv_sem=b_recv,
        device_id=mate,
        device_id_type=MESH,
    ).wait_send()
    b_moved.wait_send()


def interact(sums_ref, start_ref, dense_ref, wp_ref, pooled_ref, hidden_ref):
    samples, nt = pooled_ref.shape[0], pooled_ref.shape[1]
    pooled = sums_ref[...]
    feats = [dense_ref[...]]
    for t in range(nt):
        feats.append(pooled[t * samples : (t + 1) * samples, :])
        pooled_ref[:, t, :] = feats[-1]
    total = start_ref[...]
    pair = 0
    for one in range(nt + 1):
        for two in range(one + 1, nt + 1):
            dots = jnp.sum(feats[one] * feats[two], axis=-1, keepdims=True)
            total = total + dots * wp_ref[pair : pair + 1, :]
            pair += 1
    hidden_ref[...] = jnp.maximum(total, 0.0)


def shards(bag_index, bag_length, emb_tables, dense_feats, w_dense, w_pair, top_bias):
    samples, lanes = bag_index.shape
    nt, local_rows, width = emb_tables.shape
    cap = 2 * samples * lanes // (2 * CHIPS)
    bags = samples * nt
    units = w_dense.shape[1]
    groups = CHIPS // SIDE
    dims = (local_rows, nt, lanes // nt, cap)
    vmem = pl.BlockSpec(memory_space=pltpu.VMEM)
    anyw = pl.BlockSpec(memory_space=pltpu.HBM)
    dma = pltpu.SemaphoreType.DMA
    sums, start = pl.pallas_call(
        functools.partial(kernel, dims),
        out_shape=(
            jax.ShapeDtypeStruct((bags, width), F32),
            jax.ShapeDtypeStruct((samples, units), F32),
        ),
        in_specs=[anyw] * 6,
        out_specs=(vmem, vmem),
        scratch_shapes=[
            pltpu.VMEM((samples, lanes), I32),
            pltpu.VMEM((nt, samples), I32),
            pltpu.VMEM((samples, width), F32),
            pltpu.VMEM((1, units), F32),
            pltpu.VMEM((nt * local_rows, width), F32),
            pltpu.VMEM(w_dense.shape, F32),
            pltpu.VMEM((CHIPS, 1, 4 * cap), I32),
            pltpu.VMEM((CHIPS, 1, 4 * cap), I32),
            pltpu.SMEM((CHIPS, 1, 4 * cap), I32),
            pltpu.SMEM((CHIPS, 1, 4 * cap), I32),
            pltpu.VMEM((CHIPS, cap, width), F32),
            pltpu.VMEM((SIDE, cap, width), F32),
            pltpu.VMEM((CHIPS, cap, width), F32),
            pltpu.VMEM((CHIPS, bags, width), F32),
            pltpu.VMEM((CHIPS, bags, width), F32),
            pltpu.VMEM((groups, bags, width), F32),
            pltpu.VMEM((groups, bags, width), F32),
            dma((5,)),
            dma,
            dma,
            dma,
            dma,
            dma,
            dma,
            dma,
            dma((groups,)),
            dma,
            dma((3, TEAMS)),
            dma((3, TEAMS)),
            dma,
            dma,
        ],
        compiler_params=pltpu.CompilerParams(
            collective_id=0, has_side_effects=True, vmem_limit_bytes=40 * 1024 * 1024
        ),
    )(
        *(
            pltpu.with_memory_space_constraint(v, pltpu.HBM)
            for v in (
                bag_index,
                bag_length.T,
                emb_tables.reshape(nt * local_rows, width),
                dense_feats,
                w_dense,
                top_bias.reshape(1, units),
            )
        )
    )
    return pl.pallas_call(
        interact,
        out_shape=(
            jax.ShapeDtypeStruct((samples, nt, width), F32),
            jax.ShapeDtypeStruct((samples, units), F32),
        ),
        in_specs=[vmem] * 4,
        out_specs=(vmem, vmem),
        compiler_params=pltpu.CompilerParams(vmem_limit_bytes=8 * 1024 * 1024),
    )(sums, start, dense_feats, w_pair)


def solution(mesh):
    in_specs = (
        P(("rows", "cols"), None),
        P(("rows", "cols"), None),
        P(None, ("rows", "cols"), None),
        P(("rows", "cols"), None),
        P(),
        P(),
        P(),
    )
    out_specs = (P(("rows", "cols"), None, None), P(("rows", "cols"), None))
    return jax.shard_map(
        shards, mesh=mesh, in_specs=in_specs, out_specs=out_specs, check_vma=False
    )
```

```python
import functools

import jax
import jax.numpy as jnp
from jax import lax
from jax.experimental import pallas as pl
from jax.experimental.pallas import tpu as pltpu
from jax.sharding import PartitionSpec as P

MESH = pl.DeviceIdType.MESH
F32 = jnp.float32
BF16 = jnp.bfloat16
I32 = jnp.int32
SIDE = 4
CHIPS = SIDE**3
CHUNKS = 8
AHEAD = 5
FIRST = (16, 24, 16, 24)
SECOND = (40, 40, 48, 40)
BAGS = 64
FAR = SIDE // 2


def destinations():
    near = [1, 3, 0]
    out = []
    for far in ((1, 1, 1), (1, 1, 0), (1, 0, 1), (0, 1, 1), (1, 0, 0), (0, 1, 0), (0, 0, 1), (0, 0, 0)):
        dims = [[FAR] if f else near for f in far]
        out += [(dx, dy, dz) for dz in dims[2] for dy in dims[1] for dx in dims[0]]
    return out


ORDER = destinations()
SLOT = {d: t for t, d in enumerate(ORDER)}


def others(d, p):
    return tuple(v for q, v in enumerate(d) if q != p)


def along(p, v, o):
    return o[:p] + (v,) + o[p:]


def plane_order():
    near = [1, 3, 0]
    out = [(FAR, FAR)] + [(FAR, b) for b in near] + [(a, FAR) for a in near]
    return out + [(a, b) for b in near for a in near]


PLANE = plane_order()
PLACE = {o: g for g, o in enumerate(PLANE)}
TEAM = [0] * 4 + [1] * 3 + [2] * 3 + [3] * 3 + [4] * 3
TEAMS = 5
EARLY = {13: 0, 15: 1}


def span(p, o):
    a, b = o
    return ((0, FIRST[b]), (FIRST[b], SECOND[a]), (SECOND[a], BAGS))[p]


def height(p, planes):
    return sum(span(p, o)[1] - span(p, o)[0] for o in planes)


def joined(o):
    return 1 if sum(o) % 2 == 0 else SIDE - 1


def kernel(
    dims,
    index_hbm,
    length_hbm,
    table_hbm,
    dense_hbm,
    wd_hbm,
    bias_hbm,
    sums_ref,
    start_ref,
    index_ref,
    length_ref,
    dense_ref,
    bias_ref,
    table,
    wd,
    outbox,
    inbox,
    ids_own,
    ids_mate,
    mate_out,
    own_rows,
    mate_rows,
    a_out,
    a_in,
    b_out,
    b_in,
    input_sem,
    table_sem,
    box_send,
    box_recv,
    fwd_send,
    fwd_recv,
    own_sem,
    rows_send,
    rows_recv,
    a_send,
    far_recv,
    near_recv,
    b_send,
    b_recv,
):
    local_rows, nt, slots_bag, cap = dims
    n = 2 * CHIPS
    samples, lanes = index_ref.shape
    bags = samples * nt
    total_rows = nt * local_rows
    r = lax.axis_index("rows")
    c = lax.axis_index("cols")
    x, z, y, k = r // SIDE, r % SIDE, c // 2, c % 2

    def step_by(at, d):
        return (at + d) % SIDE

    def device(xx, yy, zz, kk):
        return {"rows": xx * SIDE + zz, "cols": yy * 2 + kk}

    offsets = sorted(ORDER, key=lambda o: -sum(min(d, SIDE - d) for d in o))

    def shifted(d, kk):
        return device(step_by(x, d[0]), step_by(y, d[1]), step_by(z, d[2]), kk)

    inputs = [
        pltpu.make_async_copy(source, target, input_sem.at[i])
        for i, (source, target) in enumerate(
            (
                (index_hbm, index_ref),
                (length_hbm, length_ref),
                (wd_hbm, wd),
                (dense_hbm, dense_ref),
                (bias_hbm, bias_ref),
            )
        )
    ]
    for copy in inputs[:2]:
        copy.start()

    mate = device(x, y, z, 1 - k)

    barrier = pltpu.get_barrier_semaphore()
    for d in offsets:
        pl.semaphore_signal(barrier, inc=1, device_id=shifted(d, 1 - k), device_id_type=MESH)
        if any(d):
            pl.semaphore_signal(barrier, inc=1, device_id=shifted(d, k), device_id_type=MESH)

    inputs[0].wait()
    inputs[1].wait()
    for copy in inputs[2:]:
        copy.start()
    part = total_rows // CHUNKS
    for i in range(CHUNKS):
        pltpu.make_async_copy(
            table_hbm.at[pl.ds(i * part, part)], table.at[pl.ds(i * part, part)], table_sem
        ).start()

    idx = index_ref[...]
    lane = lax.broadcasted_iota(I32, (samples, lanes), 1)
    table_of = lane // slots_bag
    spread = jnp.where(
        lax.broadcasted_iota(I32, (nt, lanes), 1) // slots_bag == lax.broadcasted_iota(I32, (nt, lanes), 0),
        1.0,
        0.0,
    )
    length = lax.dot_general(
        length_ref[...].astype(F32).astype(BF16),
        spread.astype(BF16),
        (((0,), (0,)), ((), ())),
        preferred_element_type=F32,
    ).astype(I32)
    live = lane - table_of * slots_bag < length
    owner = idx // local_rows
    row = table_of * local_rows + idx - owner * local_rows
    bag = table_of * samples + lax.broadcasted_iota(I32, (samples, lanes), 0)
    owner = jnp.where(live, (owner % 2) * CHIPS + owner // 2, -1)
    pieces = []
    shift = 0
    while shift == 0 or (total_rows - 1) >> shift:
        pieces.append((row // (1 << shift)) % 256)
        shift += 8
    n_row = len(pieces)
    pieces.append(bag + 1)
    pieces = [v.astype(F32) for v in pieces]
    dev_iota = lax.broadcasted_iota(I32, (n, lanes), 0)
    before = (
        lax.broadcasted_iota(I32, (lanes, lanes), 0) < lax.broadcasted_iota(I32, (lanes, lanes), 1)
    )
    before = jnp.where(before, 1.0, 0.0).astype(BF16)
    hots = [
        jnp.where(owner[b : b + 1, :] == dev_iota, 1.0, 0.0).astype(F32) for b in range(samples)
    ]
    prefix = jnp.dot(
        jnp.concatenate([h.astype(BF16) for h in hots], axis=0), before, preferred_element_type=F32
    )
    base = jnp.zeros((n, 1), F32)
    box = jnp.zeros((len(pieces) * n, cap), F32)
    cap_iota = lax.broadcasted_iota(I32, (cap, lanes), 0)
    for b in range(samples):
        hot = hots[b]
        rank = jnp.sum(hot * (prefix[b * n : (b + 1) * n, :] + base), axis=0, keepdims=True)
        base = base + jnp.sum(hot, axis=1, keepdims=True)
        spot = jnp.where(rank.astype(I32) == cap_iota, 1.0, 0.0).astype(BF16)
        coded = jnp.concatenate([hot * v[b : b + 1, :] for v in pieces], axis=0).astype(BF16)
        box = box + lax.dot_general(
            coded, spot, (((1,), (1,)), ((), ())), preferred_element_type=F32
        )
    box_row = jnp.zeros((n, cap), I32)
    for i in range(n_row):
        box_row = box_row + box[i * n : (i + 1) * n, :].astype(I32) * (1 << (8 * i))
    box_bag = box[n_row * n :, :].astype(I32) - 1
    flip = jnp.full((CHIPS, cap), k, I32) == 1
    halves = []
    for both in (box_bag, box_row):
        halves.append(jnp.where(flip, both[CHIPS:], both[:CHIPS]))
        halves.append(jnp.where(flip, both[:CHIPS], both[CHIPS:]))
    boxes = jnp.concatenate(halves, axis=1) & (total_rows - 1)
    for d in range(CHIPS):
        outbox[d] = boxes[d : d + 1, :]

    def chip(xx, yy, zz):
        return (xx * SIDE + zz) * SIDE + yy

    inbox[SLOT[(0, 0, 0)]] = outbox[chip(x, y, z)]

    pl.semaphore_wait(barrier, n - 1)

    for d in offsets:
        back = tuple((SIDE - v) % SIDE for v in d)
        source = outbox.at[chip(step_by(x, back[0]), step_by(y, back[1]), step_by(z, back[2]))]
        pltpu.make_async_remote_copy(
            src_ref=source,
            dst_ref=ids_mate.at[SLOT[d]],
            send_sem=fwd_send,
            recv_sem=fwd_recv,
            device_id=shifted(back, 1 - k),
            device_id_type=MESH,
        ).start()
        if any(d):
            pltpu.make_async_remote_copy(
                src_ref=source,
                dst_ref=inbox.at[SLOT[d]],
                send_sem=box_send,
                recv_sem=box_recv,
                device_id=shifted(back, k),
                device_id_type=MESH,
            ).start()

    for copy in inputs[2:]:
        copy.wait()
    start_ref[...] = (
        jnp.dot(
            dense_ref[...], wd[...], precision=lax.Precision.HIGHEST, preferred_element_type=F32
        )
        + bias_ref[...]
    )

    rest = pl.ds(0, CHIPS - 1)
    boxes_moved = pltpu.make_async_remote_copy(
        src_ref=outbox.at[rest],
        dst_ref=inbox.at[rest],
        send_sem=box_send,
        recv_sem=box_recv,
        device_id=mate,
        device_id_type=MESH,
    )
    mates_moved = pltpu.make_async_remote_copy(
        src_ref=outbox,
        dst_ref=ids_mate,
        send_sem=fwd_send,
        recv_sem=fwd_recv,
        device_id=mate,
        device_id_type=MESH,
    )

    def own_copy(q):
        some = pl.ds(q * (CHIPS // SIDE), CHIPS // SIDE)
        return pltpu.make_async_copy(inbox.at[some], ids_own.at[some], own_sem.at[q])

    mates_moved.wait_recv()
    pltpu.make_async_copy(table_hbm, table, table_sem).wait()

    def rows_copy(s):
        some = pl.ds(s * SIDE, SIDE)
        return pltpu.make_async_remote_copy(
            src_ref=mate_out.at[some],
            dst_ref=mate_rows.at[some],
            send_sem=rows_send,
            recv_sem=rows_recv.at[s],
            device_id=mate,
            device_id_type=MESH,
        )

    def fetch_mate(s):
        for u in range(SIDE):
            t = s * SIDE + u
            for i in range(cap):
                mate_out[t, i : i + 1, :] = table[pl.ds(ids_mate[t, 0, 3 * cap + i], 1), :]
        rows_copy(s).start()

    def fetch_own(s):
        for u in range(SIDE):
            t = s * SIDE + u
            for i in range(cap):
                own_rows[u, i : i + 1, :] = table[pl.ds(ids_own[t, 0, 2 * cap + i], 1), :]

    def fetch_ahead(s, carry):
        fetch_mate(s)
        return carry

    fetch_mate(0)
    boxes_moved.wait_recv()
    for q in range(SIDE):
        own_copy(q).start()
    lax.fori_loop(1, AHEAD, fetch_ahead, 0)
    own_copy(0).wait()
    fetch_own(0)

    bag_iota = lax.broadcasted_iota(I32, (bags, 2 * cap), 0)

    def rows_of(p, o):
        lo, hi = span(p, o)
        return pl.ds(lo, hi - lo)

    def a_copy(t, p, shift, recv):
        rows = rows_of(p, others(ORDER[t], p))
        return pltpu.make_async_remote_copy(
            src_ref=a_out.at[t, rows],
            dst_ref=a_in.at[t, rows],
            send_sem=a_send,
            recv_sem=recv,
            device_id=shifted(along(p, shift, (0, 0)), k),
            device_id_type=MESH,
        )

    def b_copy(g, p):
        return pltpu.make_async_remote_copy(
            src_ref=b_out.at[g, rows_of(p, PLANE[g])],
            dst_ref=b_in.at[g, rows_of(p, PLANE[g])],
            send_sem=b_send,
            recv_sem=b_recv,
            device_id=shifted(along(p, 0, PLANE[g]), k),
            device_id_type=MESH,
        )

    def arrived(count, sem):
        tiles, some = pl.ds(0, count // 8), pl.ds(0, 8)
        pltpu.make_async_remote_copy(
            src_ref=a_in.at[tiles, some],
            dst_ref=a_in.at[tiles, some],
            send_sem=a_send,
            recv_sem=sem,
            device_id=mate,
            device_id_type=MESH,
        ).wait_recv()

    groups = CHIPS // SIDE

    def pool(s):
        if (s + 1) % SIDE == 0 and s + 1 < groups:
            own_copy((s + 1) // SIDE).wait()
        rows_copy(s).wait_recv()
        slots = range(s * SIDE, (s + 1) * SIDE)
        for t in slots:
            found = jnp.concatenate([own_rows[t % SIDE], mate_rows[t]], axis=0)
            high = found.astype(BF16)
            low = (found - high.astype(F32)).astype(BF16)
            select = jnp.where(inbox[t, 0:1, 0 : 2 * cap] == bag_iota, 1.0, 0.0).astype(BF16)
            value = jnp.dot(select, high, preferred_element_type=F32) + jnp.dot(
                select, low, preferred_element_type=F32
            )
            a_out[t] = value
            for p in range(3):
                if ORDER[t][p] == 0:
                    lo, hi = span(p, others(ORDER[t], p))
                    a_in[t, lo:hi, :] = value[lo:hi]
        if s + 1 < groups:
            fetch_own(s + 1)
        if s + AHEAD < groups:
            fetch_mate(s + AHEAD)
        for t in slots:
            for p in range(3):
                o, v = others(ORDER[t], p), ORDER[t][p]
                team = TEAM[PLACE[o]]
                if v == FAR:
                    a_copy(t, p, joined(o), far_recv.at[p, team]).start()
                elif v and v != joined(o):
                    a_copy(t, p, v, near_recv.at[p, team]).start()

    def relay(team):
        planes = [o for o in PLANE if TEAM[PLACE[o]] == team]
        for p in range(3):
            arrived(height(p, planes), far_recv.at[p, team])
            for o in planes:
                lo, hi = span(p, o)
                t, far = SLOT[along(p, joined(o), o)], SLOT[along(p, FAR, o)]
                a_out[t, lo:hi, :] = a_out[t, lo:hi, :] + a_in[far, lo:hi, :]
                a_copy(t, p, joined(o), near_recv.at[p, team]).start()

    for s in range(groups):
        pool(s)
        if s in EARLY:
            relay(EARLY[s])
    for team in range(TEAMS):
        if team not in EARLY.values():
            relay(team)
    for team in range(TEAMS):
        planes = [o for o in PLANE if TEAM[PLACE[o]] == team]
        for p in range(3):
            arrived(2 * height(p, planes), near_recv.at[p, team])
            for o in planes:
                lo, hi = span(p, o)
                g = PLACE[o]
                total = a_in[SLOT[along(p, 0, o)], lo:hi, :]
                for v in (1, SIDE - 1):
                    total = total + a_in[SLOT[along(p, v, o)], lo:hi, :]
                if any(o):
                    b_out[g, lo:hi, :] = total
                    b_copy(g, p).start()
                else:
                    b_in[g, lo:hi, :] = total

    some = pl.ds(0, groups - 1)
    b_moved = pltpu.make_async_remote_copy(
        src_ref=b_out.at[some],
        dst_ref=b_in.at[some],
        send_sem=b_send,
        recv_sem=b_recv,
        device_id=mate,
        device_id_type=MESH,
    )
    b_moved.wait_recv()
    pooled = b_in[0]
    for g in range(1, groups):
        pooled = pooled + b_in[g]

    sums_ref[...] = pooled

    boxes_moved.wait_send()
    mates_moved.wait_send()
    pltpu.make_async_remote_copy(
        src_ref=mate_out,
        dst_ref=mate_out,
        send_sem=rows_send,
        recv_sem=b_recv,
        device_id=mate,
        device_id_type=MESH,
    ).wait_send()
    some = pl.ds(0, CHIPS - groups)
    pltpu.make_async_remote_copy(
        src_ref=a_out.at[some],
        dst_ref=a_in.at[some],
        send_sem=a_send,
        recv_sem=b_recv,
        device_id=mate,
        device_id_type=MESH,
    ).wait_send()
    b_moved.wait_send()


def interact(sums_ref, start_ref, dense_ref, wp_ref, pooled_ref, hidden_ref):
    samples, nt = pooled_ref.shape[0], pooled_ref.shape[1]
    pooled = sums_ref[...]
    feats = [dense_ref[...]]
    for t in range(nt):
        feats.append(pooled[t * samples : (t + 1) * samples, :])
        pooled_ref[:, t, :] = feats[-1]
    total = start_ref[...]
    pair = 0
    for one in range(nt + 1):
        for two in range(one + 1, nt + 1):
            dots = jnp.sum(feats[one] * feats[two], axis=-1, keepdims=True)
            total = total + dots * wp_ref[pair : pair + 1, :]
            pair += 1
    hidden_ref[...] = jnp.maximum(total, 0.0)


def shards(bag_index, bag_length, emb_tables, dense_feats, w_dense, w_pair, top_bias):
    samples, lanes = bag_index.shape
    nt, local_rows, width = emb_tables.shape
    cap = 2 * samples * lanes // (2 * CHIPS)
    bags = samples * nt
    units = w_dense.shape[1]
    groups = CHIPS // SIDE
    dims = (local_rows, nt, lanes // nt, cap)
    vmem = pl.BlockSpec(memory_space=pltpu.VMEM)
    anyw = pl.BlockSpec(memory_space=pltpu.HBM)
    dma = pltpu.SemaphoreType.DMA
    sums, start = pl.pallas_call(
        functools.partial(kernel, dims),
        out_shape=(
            jax.ShapeDtypeStruct((bags, width), F32),
            jax.ShapeDtypeStruct((samples, units), F32),
        ),
        in_specs=[anyw] * 6,
        out_specs=(vmem, vmem),
        scratch_shapes=[
            pltpu.VMEM((samples, lanes), I32),
            pltpu.VMEM((nt, samples), I32),
            pltpu.VMEM((samples, width), F32),
            pltpu.VMEM((1, units), F32),
            pltpu.VMEM((nt * local_rows, width), F32),
            pltpu.VMEM(w_dense.shape, F32),
            pltpu.VMEM((CHIPS, 1, 4 * cap), I32),
            pltpu.VMEM((CHIPS, 1, 4 * cap), I32),
            pltpu.SMEM((CHIPS, 1, 4 * cap), I32),
            pltpu.SMEM((CHIPS, 1, 4 * cap), I32),
            pltpu.VMEM((CHIPS, cap, width), F32),
            pltpu.VMEM((SIDE, cap, width), F32),
            pltpu.VMEM((CHIPS, cap, width), F32),
            pltpu.VMEM((CHIPS, bags, width), F32),
            pltpu.VMEM((CHIPS, bags, width), F32),
            pltpu.VMEM((groups, bags, width), F32),
            pltpu.VMEM((groups, bags, width), F32),
            dma((5,)),
            dma,
            dma,
            dma,
            dma,
            dma,
            dma((SIDE,)),
            dma,
            dma((groups,)),
            dma,
            dma((3, TEAMS)),
            dma((3, TEAMS)),
            dma,
            dma,
        ],
        compiler_params=pltpu.CompilerParams(
            collective_id=0, has_side_effects=True, vmem_limit_bytes=40 * 1024 * 1024
        ),
    )(
        *(
            pltpu.with_memory_space_constraint(v, pltpu.HBM)
            for v in (
                bag_index,
                bag_length.T,
                emb_tables.reshape(nt * local_rows, width),
                dense_feats,
                w_dense,
                top_bias.reshape(1, units),
            )
        )
    )
    return pl.pallas_call(
        interact,
        out_shape=(
            jax.ShapeDtypeStruct((samples, nt, width), F32),
            jax.ShapeDtypeStruct((samples, units), F32),
        ),
        in_specs=[vmem] * 4,
        out_specs=(vmem, vmem),
        compiler_params=pltpu.CompilerParams(vmem_limit_bytes=8 * 1024 * 1024),
    )(sums, start, dense_feats, w_pair)


def solution(mesh):
    in_specs = (
        P(("rows", "cols"), None),
        P(("rows", "cols"), None),
        P(None, ("rows", "cols"), None),
        P(("rows", "cols"), None),
        P(),
        P(),
        P(),
    )
    out_specs = (P(("rows", "cols"), None, None), P(("rows", "cols"), None))
    return jax.shard_map(
        shards, mesh=mesh, in_specs=in_specs, out_specs=out_specs, check_vma=False
    )
```

```python
import functools

import jax
import jax.numpy as jnp
from jax import lax
from jax.experimental import pallas as pl
from jax.experimental.pallas import tpu as pltpu
from jax.sharding import PartitionSpec as P

MESH = pl.DeviceIdType.MESH
F32 = jnp.float32
BF16 = jnp.bfloat16
I32 = jnp.int32
SIDE = 4
CHIPS = SIDE**3
CHUNKS = 8
AHEAD = 5
FIRST = (24, 24, 16, 24)
SECOND = (40, 48, 40, 48)
BAGS = 64
FAR = SIDE // 2


def destinations():
    near = [1, 3, 0]
    out = []
    for far in ((1, 1, 1), (1, 1, 0), (1, 0, 1), (0, 1, 1), (1, 0, 0), (0, 1, 0), (0, 0, 1), (0, 0, 0)):
        dims = [[FAR] if f else near for f in far]
        out += [(dx, dy, dz) for dz in dims[2] for dy in dims[1] for dx in dims[0]]
    return out


ORDER = destinations()
SLOT = {d: t for t, d in enumerate(ORDER)}


def others(d, p):
    return tuple(v for q, v in enumerate(d) if q != p)


def along(p, v, o):
    return o[:p] + (v,) + o[p:]


def plane_order():
    near = [1, 3, 0]
    out = [(FAR, FAR)] + [(FAR, b) for b in near] + [(a, FAR) for a in near]
    return out + [(a, b) for b in near for a in near]


PLANE = plane_order()
PLACE = {o: g for g, o in enumerate(PLANE)}
TEAM = [0] * 4 + [1] * 3 + [2] * 3 + [3] * 3 + [4] * 3
TEAMS = 5
EARLY = {13: 0, 15: 1}


def span(p, o):
    a, b = o
    return ((0, FIRST[b]), (FIRST[b], SECOND[a]), (SECOND[a], BAGS))[p]


def height(p, planes):
    return sum(span(p, o)[1] - span(p, o)[0] for o in planes)


def joined(o):
    return 1 if sum(o) % 2 == 0 else SIDE - 1


def kernel(
    dims,
    index_hbm,
    length_hbm,
    table_hbm,
    dense_hbm,
    wd_hbm,
    bias_hbm,
    sums_ref,
    start_ref,
    index_ref,
    length_ref,
    dense_ref,
    bias_ref,
    table,
    wd,
    outbox,
    inbox,
    ids_own,
    ids_mate,
    mate_out,
    own_rows,
    mate_rows,
    a_out,
    a_in,
    b_out,
    b_in,
    input_sem,
    table_sem,
    box_send,
    box_recv,
    fwd_send,
    fwd_recv,
    own_sem,
    rows_send,
    rows_recv,
    a_send,
    far_recv,
    near_recv,
    b_send,
    b_recv,
):
    local_rows, nt, slots_bag, cap = dims
    n = 2 * CHIPS
    samples, lanes = index_ref.shape
    bags = samples * nt
    total_rows = nt * local_rows
    r = lax.axis_index("rows")
    c = lax.axis_index("cols")
    x, z, y, k = r // SIDE, r % SIDE, c // 2, c % 2

    def step_by(at, d):
        return (at + d) % SIDE

    def device(xx, yy, zz, kk):
        return {"rows": xx * SIDE + zz, "cols": yy * 2 + kk}

    offsets = sorted(ORDER, key=lambda o: -sum(min(d, SIDE - d) for d in o))

    def shifted(d, kk):
        return device(step_by(x, d[0]), step_by(y, d[1]), step_by(z, d[2]), kk)

    inputs = [
        pltpu.make_async_copy(source, target, input_sem.at[i])
        for i, (source, target) in enumerate(
            (
                (index_hbm, index_ref),
                (length_hbm, length_ref),
                (wd_hbm, wd),
                (dense_hbm, dense_ref),
                (bias_hbm, bias_ref),
            )
        )
    ]
    for copy in inputs[:2]:
        copy.start()

    mate = device(x, y, z, 1 - k)

    barrier = pltpu.get_barrier_semaphore()
    for d in offsets:
        pl.semaphore_signal(barrier, inc=1, device_id=shifted(d, 1 - k), device_id_type=MESH)
        if any(d):
            pl.semaphore_signal(barrier, inc=1, device_id=shifted(d, k), device_id_type=MESH)

    inputs[0].wait()
    inputs[1].wait()
    for copy in inputs[2:]:
        copy.start()
    part = total_rows // CHUNKS
    for i in range(CHUNKS):
        pltpu.make_async_copy(
            table_hbm.at[pl.ds(i * part, part)], table.at[pl.ds(i * part, part)], table_sem
        ).start()

    idx = index_ref[...]
    lane = lax.broadcasted_iota(I32, (samples, lanes), 1)
    table_of = lane // slots_bag
    spread = jnp.where(
        lax.broadcasted_iota(I32, (nt, lanes), 1) // slots_bag == lax.broadcasted_iota(I32, (nt, lanes), 0),
        1.0,
        0.0,
    )
    length = lax.dot_general(
        length_ref[...].astype(F32).astype(BF16),
        spread.astype(BF16),
        (((0,), (0,)), ((), ())),
        preferred_element_type=F32,
    ).astype(I32)
    live = lane - table_of * slots_bag < length
    owner = idx // local_rows
    row = table_of * local_rows + idx - owner * local_rows
    bag = table_of * samples + lax.broadcasted_iota(I32, (samples, lanes), 0)
    owner = jnp.where(live, (owner % 2) * CHIPS + owner // 2, -1)
    pieces = []
    shift = 0
    while shift == 0 or (total_rows - 1) >> shift:
        pieces.append((row // (1 << shift)) % 256)
        shift += 8
    n_row = len(pieces)
    pieces.append(bag + 1)
    pieces = [v.astype(F32) for v in pieces]
    dev_iota = lax.broadcasted_iota(I32, (n, lanes), 0)
    before = (
        lax.broadcasted_iota(I32, (lanes, lanes), 0) < lax.broadcasted_iota(I32, (lanes, lanes), 1)
    )
    before = jnp.where(before, 1.0, 0.0).astype(BF16)
    hots = [
        jnp.where(owner[b : b + 1, :] == dev_iota, 1.0, 0.0).astype(F32) for b in range(samples)
    ]
    prefix = jnp.dot(
        jnp.concatenate([h.astype(BF16) for h in hots], axis=0), before, preferred_element_type=F32
    )
    base = jnp.zeros((n, 1), F32)
    box = jnp.zeros((len(pieces) * n, cap), F32)
    cap_iota = lax.broadcasted_iota(I32, (cap, lanes), 0)
    for b in range(samples):
        hot = hots[b]
        rank = jnp.sum(hot * (prefix[b * n : (b + 1) * n, :] + base), axis=0, keepdims=True)
        base = base + jnp.sum(hot, axis=1, keepdims=True)
        spot = jnp.where(rank.astype(I32) == cap_iota, 1.0, 0.0).astype(BF16)
        coded = jnp.concatenate([hot * v[b : b + 1, :] for v in pieces], axis=0).astype(BF16)
        box = box + lax.dot_general(
            coded, spot, (((1,), (1,)), ((), ())), preferred_element_type=F32
        )
    box_row = jnp.zeros((n, cap), I32)
    for i in range(n_row):
        box_row = box_row + box[i * n : (i + 1) * n, :].astype(I32) * (1 << (8 * i))
    box_bag = box[n_row * n :, :].astype(I32) - 1
    flip = jnp.full((CHIPS, cap), k, I32) == 1
    halves = []
    for both in (box_bag, box_row):
        halves.append(jnp.where(flip, both[CHIPS:], both[:CHIPS]))
        halves.append(jnp.where(flip, both[:CHIPS], both[CHIPS:]))
    boxes = jnp.concatenate(halves, axis=1) & (total_rows - 1)
    for d in range(CHIPS):
        outbox[d] = boxes[d : d + 1, :]

    def chip(xx, yy, zz):
        return (xx * SIDE + zz) * SIDE + yy

    inbox[SLOT[(0, 0, 0)]] = outbox[chip(x, y, z)]

    pl.semaphore_wait(barrier, n - 1)

    for d in offsets:
        back = tuple((SIDE - v) % SIDE for v in d)
        source = outbox.at[chip(step_by(x, back[0]), step_by(y, back[1]), step_by(z, back[2]))]
        pltpu.make_async_remote_copy(
            src_ref=source,
            dst_ref=ids_mate.at[SLOT[d]],
            send_sem=fwd_send,
            recv_sem=fwd_recv,
            device_id=shifted(back, 1 - k),
            device_id_type=MESH,
        ).start()
        if any(d):
            pltpu.make_async_remote_copy(
                src_ref=source,
                dst_ref=inbox.at[SLOT[d]],
                send_sem=box_send,
                recv_sem=box_recv,
                device_id=shifted(back, k),
                device_id_type=MESH,
            ).start()

    for copy in inputs[2:]:
        copy.wait()
    start_ref[...] = (
        jnp.dot(
            dense_ref[...], wd[...], precision=lax.Precision.HIGHEST, preferred_element_type=F32
        )
        + bias_ref[...]
    )

    rest = pl.ds(0, CHIPS - 1)
    boxes_moved = pltpu.make_async_remote_copy(
        src_ref=outbox.at[rest],
        dst_ref=inbox.at[rest],
        send_sem=box_send,
        recv_sem=box_recv,
        device_id=mate,
        device_id_type=MESH,
    )
    mates_moved = pltpu.make_async_remote_copy(
        src_ref=outbox,
        dst_ref=ids_mate,
        send_sem=fwd_send,
        recv_sem=fwd_recv,
        device_id=mate,
        device_id_type=MESH,
    )

    def own_copy(q):
        some = pl.ds(q * (CHIPS // SIDE), CHIPS // SIDE)
        return pltpu.make_async_copy(inbox.at[some], ids_own.at[some], own_sem.at[q])

    mates_moved.wait_recv()
    pltpu.make_async_copy(table_hbm, table, table_sem).wait()

    def rows_copy(s):
        some = pl.ds(s * SIDE, SIDE)
        return pltpu.make_async_remote_copy(
            src_ref=mate_out.at[some],
            dst_ref=mate_rows.at[some],
            send_sem=rows_send,
            recv_sem=rows_recv.at[s],
            device_id=mate,
            device_id_type=MESH,
        )

    def fetch_mate(s):
        for u in range(SIDE):
            t = s * SIDE + u
            for i in range(cap):
                mate_out[t, i : i + 1, :] = table[pl.ds(ids_mate[t, 0, 3 * cap + i], 1), :]
        rows_copy(s).start()

    def fetch_own(s):
        for u in range(SIDE):
            t = s * SIDE + u
            for i in range(cap):
                own_rows[u, i : i + 1, :] = table[pl.ds(ids_own[t, 0, 2 * cap + i], 1), :]

    def fetch_ahead(s, carry):
        fetch_mate(s)
        return carry

    fetch_mate(0)
    boxes_moved.wait_recv()
    for q in range(SIDE):
        own_copy(q).start()
    lax.fori_loop(1, AHEAD, fetch_ahead, 0)
    own_copy(0).wait()
    fetch_own(0)

    bag_iota = lax.broadcasted_iota(I32, (bags, 2 * cap), 0)

    def rows_of(p, o):
        lo, hi = span(p, o)
        return pl.ds(lo, hi - lo)

    def a_copy(t, p, shift, recv):
        rows = rows_of(p, others(ORDER[t], p))
        return pltpu.make_async_remote_copy(
            src_ref=a_out.at[t, rows],
            dst_ref=a_in.at[t, rows],
            send_sem=a_send,
            recv_sem=recv,
            device_id=shifted(along(p, shift, (0, 0)), k),
            device_id_type=MESH,
        )

    def b_copy(g, p):
        return pltpu.make_async_remote_copy(
            src_ref=b_out.at[g, rows_of(p, PLANE[g])],
            dst_ref=b_in.at[g, rows_of(p, PLANE[g])],
            send_sem=b_send,
            recv_sem=b_recv,
            device_id=shifted(along(p, 0, PLANE[g]), k),
            device_id_type=MESH,
        )

    def arrived(count, sem):
        tiles, some = pl.ds(0, count // 8), pl.ds(0, 8)
        pltpu.make_async_remote_copy(
            src_ref=a_in.at[tiles, some],
            dst_ref=a_in.at[tiles, some],
            send_sem=a_send,
            recv_sem=sem,
            device_id=mate,
            device_id_type=MESH,
        ).wait_recv()

    groups = CHIPS // SIDE

    def pool(s):
        if (s + 1) % SIDE == 0 and s + 1 < groups:
            own_copy((s + 1) // SIDE).wait()
        rows_copy(s).wait_recv()
        slots = range(s * SIDE, (s + 1) * SIDE)
        for t in slots:
            found = jnp.concatenate([own_rows[t % SIDE], mate_rows[t]], axis=0)
            high = found.astype(BF16)
            low = (found - high.astype(F32)).astype(BF16)
            select = jnp.where(inbox[t, 0:1, 0 : 2 * cap] == bag_iota, 1.0, 0.0).astype(BF16)
            value = jnp.dot(select, high, preferred_element_type=F32) + jnp.dot(
                select, low, preferred_element_type=F32
            )
            a_out[t] = value
            for p in range(3):
                if ORDER[t][p] == 0:
                    lo, hi = span(p, others(ORDER[t], p))
                    a_in[t, lo:hi, :] = value[lo:hi]
        if s + 1 < groups:
            fetch_own(s + 1)
        if s + AHEAD < groups:
            fetch_mate(s + AHEAD)
        for t in slots:
            for p in range(3):
                o, v = others(ORDER[t], p), ORDER[t][p]
                team = TEAM[PLACE[o]]
                if v == FAR:
                    a_copy(t, p, joined(o), far_recv.at[p, team]).start()
                elif v and v != joined(o):
                    a_copy(t, p, v, near_recv.at[p, team]).start()

    def relay(team):
        planes = [o for o in PLANE if TEAM[PLACE[o]] == team]
        for p in range(3):
            arrived(height(p, planes), far_recv.at[p, team])
            for o in planes:
                lo, hi = span(p, o)
                t, far = SLOT[along(p, joined(o), o)], SLOT[along(p, FAR, o)]
                a_out[t, lo:hi, :] = a_out[t, lo:hi, :] + a_in[far, lo:hi, :]
                a_copy(t, p, joined(o), near_recv.at[p, team]).start()

    for s in range(groups):
        pool(s)
        if s in EARLY:
            relay(EARLY[s])
    for team in range(TEAMS):
        if team not in EARLY.values():
            relay(team)
    for team in range(TEAMS):
        planes = [o for o in PLANE if TEAM[PLACE[o]] == team]
        for p in range(3):
            arrived(2 * height(p, planes), near_recv.at[p, team])
            for o in planes:
                lo, hi = span(p, o)
                g = PLACE[o]
                total = a_in[SLOT[along(p, 0, o)], lo:hi, :]
                for v in (1, SIDE - 1):
                    total = total + a_in[SLOT[along(p, v, o)], lo:hi, :]
                if any(o):
                    b_out[g, lo:hi, :] = total
                    b_copy(g, p).start()
                else:
                    b_in[g, lo:hi, :] = total

    some = pl.ds(0, groups - 1)
    b_moved = pltpu.make_async_remote_copy(
        src_ref=b_out.at[some],
        dst_ref=b_in.at[some],
        send_sem=b_send,
        recv_sem=b_recv,
        device_id=mate,
        device_id_type=MESH,
    )
    b_moved.wait_recv()
    pooled = b_in[0]
    for g in range(1, groups):
        pooled = pooled + b_in[g]

    sums_ref[...] = pooled

    boxes_moved.wait_send()
    mates_moved.wait_send()
    pltpu.make_async_remote_copy(
        src_ref=mate_out,
        dst_ref=mate_out,
        send_sem=rows_send,
        recv_sem=b_recv,
        device_id=mate,
        device_id_type=MESH,
    ).wait_send()
    some = pl.ds(0, CHIPS - groups)
    pltpu.make_async_remote_copy(
        src_ref=a_out.at[some],
        dst_ref=a_in.at[some],
        send_sem=a_send,
        recv_sem=b_recv,
        device_id=mate,
        device_id_type=MESH,
    ).wait_send()
    b_moved.wait_send()


def interact(sums_ref, start_ref, dense_ref, wp_ref, pooled_ref, hidden_ref):
    samples, nt = pooled_ref.shape[0], pooled_ref.shape[1]
    pooled = sums_ref[...]
    feats = [dense_ref[...]]
    for t in range(nt):
        feats.append(pooled[t * samples : (t + 1) * samples, :])
        pooled_ref[:, t, :] = feats[-1]
    total = start_ref[...]
    pair = 0
    for one in range(nt + 1):
        for two in range(one + 1, nt + 1):
            dots = jnp.sum(feats[one] * feats[two], axis=-1, keepdims=True)
            total = total + dots * wp_ref[pair : pair + 1, :]
            pair += 1
    hidden_ref[...] = jnp.maximum(total, 0.0)


def shards(bag_index, bag_length, emb_tables, dense_feats, w_dense, w_pair, top_bias):
    samples, lanes = bag_index.shape
    nt, local_rows, width = emb_tables.shape
    cap = 2 * samples * lanes // (2 * CHIPS)
    bags = samples * nt
    units = w_dense.shape[1]
    groups = CHIPS // SIDE
    dims = (local_rows, nt, lanes // nt, cap)
    vmem = pl.BlockSpec(memory_space=pltpu.VMEM)
    anyw = pl.BlockSpec(memory_space=pltpu.HBM)
    dma = pltpu.SemaphoreType.DMA
    sums, start = pl.pallas_call(
        functools.partial(kernel, dims),
        out_shape=(
            jax.ShapeDtypeStruct((bags, width), F32),
            jax.ShapeDtypeStruct((samples, units), F32),
        ),
        in_specs=[anyw] * 6,
        out_specs=(vmem, vmem),
        scratch_shapes=[
            pltpu.VMEM((samples, lanes), I32),
            pltpu.VMEM((nt, samples), I32),
            pltpu.VMEM((samples, width), F32),
            pltpu.VMEM((1, units), F32),
            pltpu.VMEM((nt * local_rows, width), F32),
            pltpu.VMEM(w_dense.shape, F32),
            pltpu.VMEM((CHIPS, 1, 4 * cap), I32),
            pltpu.VMEM((CHIPS, 1, 4 * cap), I32),
            pltpu.SMEM((CHIPS, 1, 4 * cap), I32),
            pltpu.SMEM((CHIPS, 1, 4 * cap), I32),
            pltpu.VMEM((CHIPS, cap, width), F32),
            pltpu.VMEM((SIDE, cap, width), F32),
            pltpu.VMEM((CHIPS, cap, width), F32),
            pltpu.VMEM((CHIPS, bags, width), F32),
            pltpu.VMEM((CHIPS, bags, width), F32),
            pltpu.VMEM((groups, bags, width), F32),
            pltpu.VMEM((groups, bags, width), F32),
            dma((5,)),
            dma,
            dma,
            dma,
            dma,
            dma,
            dma((SIDE,)),
            dma,
            dma((groups,)),
            dma,
            dma((3, TEAMS)),
            dma((3, TEAMS)),
            dma,
            dma,
        ],
        compiler_params=pltpu.CompilerParams(
            collective_id=0, has_side_effects=True, vmem_limit_bytes=40 * 1024 * 1024
        ),
    )(
        *(
            pltpu.with_memory_space_constraint(v, pltpu.HBM)
            for v in (
                bag_index,
                bag_length.T,
                emb_tables.reshape(nt * local_rows, width),
                dense_feats,
                w_dense,
                top_bias.reshape(1, units),
            )
        )
    )
    return pl.pallas_call(
        interact,
        out_shape=(
            jax.ShapeDtypeStruct((samples, nt, width), F32),
            jax.ShapeDtypeStruct((samples, units), F32),
        ),
        in_specs=[vmem] * 4,
        out_specs=(vmem, vmem),
        compiler_params=pltpu.CompilerParams(vmem_limit_bytes=8 * 1024 * 1024),
    )(sums, start, dense_feats, w_pair)


def solution(mesh):
    in_specs = (
        P(("rows", "cols"), None),
        P(("rows", "cols"), None),
        P(None, ("rows", "cols"), None),
        P(("rows", "cols"), None),
        P(),
        P(),
        P(),
    )
    out_specs = (P(("rows", "cols"), None, None), P(("rows", "cols"), None))
    return jax.shard_map(
        shards, mesh=mesh, in_specs=in_specs, out_specs=out_specs, check_vma=False
    )
```

```python
import functools

import jax
import jax.numpy as jnp
from jax import lax
from jax.experimental import pallas as pl
from jax.experimental.pallas import tpu as pltpu
from jax.sharding import PartitionSpec as P

MESH = pl.DeviceIdType.MESH
F32 = jnp.float32
BF16 = jnp.bfloat16
I32 = jnp.int32
SIDE = 4
CHIPS = SIDE**3
CHUNKS = 8
AHEAD = 6
FIRST = (24, 24, 16, 24)
SECOND = (40, 48, 40, 48)
BAGS = 64
FAR = SIDE // 2


def destinations():
    near = [1, 3, 0]
    out = []
    for far in ((1, 1, 1), (1, 1, 0), (1, 0, 1), (0, 1, 1), (1, 0, 0), (0, 1, 0), (0, 0, 1), (0, 0, 0)):
        dims = [[FAR] if f else near for f in far]
        out += [(dx, dy, dz) for dz in dims[2] for dy in dims[1] for dx in dims[0]]
    return out


ORDER = destinations()
SLOT = {d: t for t, d in enumerate(ORDER)}


def others(d, p):
    return tuple(v for q, v in enumerate(d) if q != p)


def along(p, v, o):
    return o[:p] + (v,) + o[p:]


def plane_order():
    near = [1, 3, 0]
    out = [(FAR, FAR)] + [(FAR, b) for b in near] + [(a, FAR) for a in near]
    return out + [(a, b) for b in near for a in near]


PLANE = plane_order()
PLACE = {o: g for g, o in enumerate(PLANE)}
TEAM = [0] * 4 + [1] * 3 + [2] * 3 + [3] * 3 + [4] * 3
TEAMS = 5
EARLY = {13: 0, 15: 1}


def span(p, o):
    a, b = o
    return ((0, FIRST[b]), (FIRST[b], SECOND[a]), (SECOND[a], BAGS))[p]


def height(p, planes):
    return sum(span(p, o)[1] - span(p, o)[0] for o in planes)


def joined(o):
    return 1 if sum(o) % 2 == 0 else SIDE - 1


def kernel(
    dims,
    index_hbm,
    length_hbm,
    table_hbm,
    dense_hbm,
    wd_hbm,
    bias_hbm,
    sums_ref,
    start_ref,
    index_ref,
    length_ref,
    dense_ref,
    bias_ref,
    table,
    wd,
    outbox,
    inbox,
    ids_own,
    ids_mate,
    mate_out,
    own_rows,
    mate_rows,
    a_out,
    a_in,
    b_out,
    b_in,
    input_sem,
    table_sem,
    box_send,
    box_recv,
    fwd_send,
    fwd_recv,
    own_sem,
    rows_send,
    rows_recv,
    a_send,
    far_recv,
    near_recv,
    b_send,
    b_recv,
):
    local_rows, nt, slots_bag, cap = dims
    n = 2 * CHIPS
    samples, lanes = index_ref.shape
    bags = samples * nt
    total_rows = nt * local_rows
    r = lax.axis_index("rows")
    c = lax.axis_index("cols")
    x, z, y, k = r // SIDE, r % SIDE, c // 2, c % 2

    def step_by(at, d):
        return (at + d) % SIDE

    def device(xx, yy, zz, kk):
        return {"rows": xx * SIDE + zz, "cols": yy * 2 + kk}

    offsets = sorted(ORDER, key=lambda o: -sum(min(d, SIDE - d) for d in o))

    def shifted(d, kk):
        return device(step_by(x, d[0]), step_by(y, d[1]), step_by(z, d[2]), kk)

    inputs = [
        pltpu.make_async_copy(source, target, input_sem.at[i])
        for i, (source, target) in enumerate(
            (
                (index_hbm, index_ref),
                (length_hbm, length_ref),
                (wd_hbm, wd),
                (dense_hbm, dense_ref),
                (bias_hbm, bias_ref),
            )
        )
    ]
    for copy in inputs[:2]:
        copy.start()

    mate = device(x, y, z, 1 - k)

    barrier = pltpu.get_barrier_semaphore()
    for d in offsets:
        pl.semaphore_signal(barrier, inc=1, device_id=shifted(d, 1 - k), device_id_type=MESH)
        if any(d):
            pl.semaphore_signal(barrier, inc=1, device_id=shifted(d, k), device_id_type=MESH)

    inputs[0].wait()
    inputs[1].wait()
    for copy in inputs[2:]:
        copy.start()
    part = total_rows // CHUNKS
    for i in range(CHUNKS):
        pltpu.make_async_copy(
            table_hbm.at[pl.ds(i * part, part)], table.at[pl.ds(i * part, part)], table_sem
        ).start()

    idx = index_ref[...]
    lane = lax.broadcasted_iota(I32, (samples, lanes), 1)
    table_of = lane // slots_bag
    spread = jnp.where(
        lax.broadcasted_iota(I32, (nt, lanes), 1) // slots_bag == lax.broadcasted_iota(I32, (nt, lanes), 0),
        1.0,
        0.0,
    )
    length = lax.dot_general(
        length_ref[...].astype(F32).astype(BF16),
        spread.astype(BF16),
        (((0,), (0,)), ((), ())),
        preferred_element_type=F32,
    ).astype(I32)
    live = lane - table_of * slots_bag < length
    owner = idx // local_rows
    row = table_of * local_rows + idx - owner * local_rows
    bag = table_of * samples + lax.broadcasted_iota(I32, (samples, lanes), 0)
    owner = jnp.where(live, (owner % 2) * CHIPS + owner // 2, -1)
    pieces = []
    shift = 0
    while shift == 0 or (total_rows - 1) >> shift:
        pieces.append((row // (1 << shift)) % 256)
        shift += 8
    n_row = len(pieces)
    pieces.append(bag + 1)
    pieces = [v.astype(F32) for v in pieces]
    dev_iota = lax.broadcasted_iota(I32, (n, lanes), 0)
    before = (
        lax.broadcasted_iota(I32, (lanes, lanes), 0) < lax.broadcasted_iota(I32, (lanes, lanes), 1)
    )
    before = jnp.where(before, 1.0, 0.0).astype(BF16)
    hots = [
        jnp.where(owner[b : b + 1, :] == dev_iota, 1.0, 0.0).astype(F32) for b in range(samples)
    ]
    prefix = jnp.dot(
        jnp.concatenate([h.astype(BF16) for h in hots], axis=0), before, preferred_element_type=F32
    )
    base = jnp.zeros((n, 1), F32)
    box = jnp.zeros((len(pieces) * n, cap), F32)
    cap_iota = lax.broadcasted_iota(I32, (cap, lanes), 0)
    for b in range(samples):
        hot = hots[b]
        rank = jnp.sum(hot * (prefix[b * n : (b + 1) * n, :] + base), axis=0, keepdims=True)
        base = base + jnp.sum(hot, axis=1, keepdims=True)
        spot = jnp.where(rank.astype(I32) == cap_iota, 1.0, 0.0).astype(BF16)
        coded = jnp.concatenate([hot * v[b : b + 1, :] for v in pieces], axis=0).astype(BF16)
        box = box + lax.dot_general(
            coded, spot, (((1,), (1,)), ((), ())), preferred_element_type=F32
        )
    box_row = jnp.zeros((n, cap), I32)
    for i in range(n_row):
        box_row = box_row + box[i * n : (i + 1) * n, :].astype(I32) * (1 << (8 * i))
    box_bag = box[n_row * n :, :].astype(I32) - 1
    flip = jnp.full((CHIPS, cap), k, I32) == 1
    halves = []
    for both in (box_bag, box_row):
        halves.append(jnp.where(flip, both[CHIPS:], both[:CHIPS]))
        halves.append(jnp.where(flip, both[:CHIPS], both[CHIPS:]))
    boxes = jnp.concatenate(halves, axis=1) & (total_rows - 1)
    for d in range(CHIPS):
        outbox[d] = boxes[d : d + 1, :]

    def chip(xx, yy, zz):
        return (xx * SIDE + zz) * SIDE + yy

    inbox[SLOT[(0, 0, 0)]] = outbox[chip(x, y, z)]

    pl.semaphore_wait(barrier, n - 1)

    for d in offsets:
        back = tuple((SIDE - v) % SIDE for v in d)
        source = outbox.at[chip(step_by(x, back[0]), step_by(y, back[1]), step_by(z, back[2]))]
        pltpu.make_async_remote_copy(
            src_ref=source,
            dst_ref=ids_mate.at[SLOT[d]],
            send_sem=fwd_send,
            recv_sem=fwd_recv,
            device_id=shifted(back, 1 - k),
            device_id_type=MESH,
        ).start()
        if any(d):
            pltpu.make_async_remote_copy(
                src_ref=source,
                dst_ref=inbox.at[SLOT[d]],
                send_sem=box_send,
                recv_sem=box_recv,
                device_id=shifted(back, k),
                device_id_type=MESH,
            ).start()

    for copy in inputs[2:]:
        copy.wait()
    start_ref[...] = (
        jnp.dot(
            dense_ref[...], wd[...], precision=lax.Precision.HIGHEST, preferred_element_type=F32
        )
        + bias_ref[...]
    )

    rest = pl.ds(0, CHIPS - 1)
    boxes_moved = pltpu.make_async_remote_copy(
        src_ref=outbox.at[rest],
        dst_ref=inbox.at[rest],
        send_sem=box_send,
        recv_sem=box_recv,
        device_id=mate,
        device_id_type=MESH,
    )
    mates_moved = pltpu.make_async_remote_copy(
        src_ref=outbox,
        dst_ref=ids_mate,
        send_sem=fwd_send,
        recv_sem=fwd_recv,
        device_id=mate,
        device_id_type=MESH,
    )

    def own_copy(q):
        some = pl.ds(q * (CHIPS // SIDE), CHIPS // SIDE)
        return pltpu.make_async_copy(inbox.at[some], ids_own.at[some], own_sem.at[q])

    mates_moved.wait_recv()
    pltpu.make_async_copy(table_hbm, table, table_sem).wait()

    def rows_copy(s):
        some = pl.ds(s * SIDE, SIDE)
        return pltpu.make_async_remote_copy(
            src_ref=mate_out.at[some],
            dst_ref=mate_rows.at[some],
            send_sem=rows_send,
            recv_sem=rows_recv.at[s],
            device_id=mate,
            device_id_type=MESH,
        )

    def fetch_mate(s):
        for u in range(SIDE):
            t = s * SIDE + u
            for i in range(cap):
                mate_out[t, i : i + 1, :] = table[pl.ds(ids_mate[t, 0, 3 * cap + i], 1), :]
        rows_copy(s).start()

    def fetch_own(s):
        for u in range(SIDE):
            t = s * SIDE + u
            for i in range(cap):
                own_rows[u, i : i + 1, :] = table[pl.ds(ids_own[t, 0, 2 * cap + i], 1), :]

    def fetch_ahead(s, carry):
        fetch_mate(s)
        return carry

    fetch_mate(0)
    boxes_moved.wait_recv()
    for q in range(SIDE):
        own_copy(q).start()
    lax.fori_loop(1, AHEAD, fetch_ahead, 0)
    own_copy(0).wait()
    fetch_own(0)

    bag_iota = lax.broadcasted_iota(I32, (bags, 2 * cap), 0)

    def rows_of(p, o):
        lo, hi = span(p, o)
        return pl.ds(lo, hi - lo)

    def a_copy(t, p, shift, recv):
        rows = rows_of(p, others(ORDER[t], p))
        return pltpu.make_async_remote_copy(
            src_ref=a_out.at[t, rows],
            dst_ref=a_in.at[t, rows],
            send_sem=a_send,
            recv_sem=recv,
            device_id=shifted(along(p, shift, (0, 0)), k),
            device_id_type=MESH,
        )

    def b_copy(g, p):
        return pltpu.make_async_remote_copy(
            src_ref=b_out.at[g, rows_of(p, PLANE[g])],
            dst_ref=b_in.at[g, rows_of(p, PLANE[g])],
            send_sem=b_send,
            recv_sem=b_recv,
            device_id=shifted(along(p, 0, PLANE[g]), k),
            device_id_type=MESH,
        )

    def arrived(count, sem):
        tiles, some = pl.ds(0, count // 8), pl.ds(0, 8)
        pltpu.make_async_remote_copy(
            src_ref=a_in.at[tiles, some],
            dst_ref=a_in.at[tiles, some],
            send_sem=a_send,
            recv_sem=sem,
            device_id=mate,
            device_id_type=MESH,
        ).wait_recv()

    groups = CHIPS // SIDE

    def pool(s):
        if (s + 1) % SIDE == 0 and s + 1 < groups:
            own_copy((s + 1) // SIDE).wait()
        rows_copy(s).wait_recv()
        slots = range(s * SIDE, (s + 1) * SIDE)
        for t in slots:
            found = jnp.concatenate([own_rows[t % SIDE], mate_rows[t]], axis=0)
            high = found.astype(BF16)
            low = (found - high.astype(F32)).astype(BF16)
            select = jnp.where(inbox[t, 0:1, 0 : 2 * cap] == bag_iota, 1.0, 0.0).astype(BF16)
            value = jnp.dot(select, high, preferred_element_type=F32) + jnp.dot(
                select, low, preferred_element_type=F32
            )
            a_out[t] = value
            for p in range(3):
                if ORDER[t][p] == 0:
                    lo, hi = span(p, others(ORDER[t], p))
                    a_in[t, lo:hi, :] = value[lo:hi]
        if s + 1 < groups:
            fetch_own(s + 1)
        if s + AHEAD < groups:
            fetch_mate(s + AHEAD)
        for t in slots:
            for p in range(3):
                o, v = others(ORDER[t], p), ORDER[t][p]
                team = TEAM[PLACE[o]]
                if v == FAR:
                    a_copy(t, p, joined(o), far_recv.at[p, team]).start()
                elif v and v != joined(o):
                    a_copy(t, p, v, near_recv.at[p, team]).start()

    def relay(team):
        planes = [o for o in PLANE if TEAM[PLACE[o]] == team]
        for p in range(3):
            arrived(height(p, planes), far_recv.at[p, team])
            for o in planes:
                lo, hi = span(p, o)
                t, far = SLOT[along(p, joined(o), o)], SLOT[along(p, FAR, o)]
                a_out[t, lo:hi, :] = a_out[t, lo:hi, :] + a_in[far, lo:hi, :]
                a_copy(t, p, joined(o), near_recv.at[p, team]).start()

    for s in range(groups):
        pool(s)
        if s in EARLY:
            relay(EARLY[s])
    for team in range(TEAMS):
        if team not in EARLY.values():
            relay(team)
    for team in range(TEAMS):
        planes = [o for o in PLANE if TEAM[PLACE[o]] == team]
        for p in range(3):
            arrived(2 * height(p, planes), near_recv.at[p, team])
            for o in planes:
                lo, hi = span(p, o)
                g = PLACE[o]
                total = a_in[SLOT[along(p, 0, o)], lo:hi, :]
                for v in (1, SIDE - 1):
                    total = total + a_in[SLOT[along(p, v, o)], lo:hi, :]
                if any(o):
                    b_out[g, lo:hi, :] = total
                    b_copy(g, p).start()
                else:
                    b_in[g, lo:hi, :] = total

    some = pl.ds(0, groups - 1)
    b_moved = pltpu.make_async_remote_copy(
        src_ref=b_out.at[some],
        dst_ref=b_in.at[some],
        send_sem=b_send,
        recv_sem=b_recv,
        device_id=mate,
        device_id_type=MESH,
    )
    b_moved.wait_recv()
    pooled = b_in[0]
    for g in range(1, groups):
        pooled = pooled + b_in[g]

    sums_ref[...] = pooled

    boxes_moved.wait_send()
    mates_moved.wait_send()
    pltpu.make_async_remote_copy(
        src_ref=mate_out,
        dst_ref=mate_out,
        send_sem=rows_send,
        recv_sem=b_recv,
        device_id=mate,
        device_id_type=MESH,
    ).wait_send()
    some = pl.ds(0, CHIPS - groups)
    pltpu.make_async_remote_copy(
        src_ref=a_out.at[some],
        dst_ref=a_in.at[some],
        send_sem=a_send,
        recv_sem=b_recv,
        device_id=mate,
        device_id_type=MESH,
    ).wait_send()
    b_moved.wait_send()


def interact(sums_ref, start_ref, dense_ref, wp_ref, pooled_ref, hidden_ref):
    samples, nt = pooled_ref.shape[0], pooled_ref.shape[1]
    pooled = sums_ref[...]
    feats = [dense_ref[...]]
    for t in range(nt):
        feats.append(pooled[t * samples : (t + 1) * samples, :])
        pooled_ref[:, t, :] = feats[-1]
    total = start_ref[...]
    pair = 0
    for one in range(nt + 1):
        for two in range(one + 1, nt + 1):
            dots = jnp.sum(feats[one] * feats[two], axis=-1, keepdims=True)
            total = total + dots * wp_ref[pair : pair + 1, :]
            pair += 1
    hidden_ref[...] = jnp.maximum(total, 0.0)


def shards(bag_index, bag_length, emb_tables, dense_feats, w_dense, w_pair, top_bias):
    samples, lanes = bag_index.shape
    nt, local_rows, width = emb_tables.shape
    cap = 2 * samples * lanes // (2 * CHIPS)
    bags = samples * nt
    units = w_dense.shape[1]
    groups = CHIPS // SIDE
    dims = (local_rows, nt, lanes // nt, cap)
    vmem = pl.BlockSpec(memory_space=pltpu.VMEM)
    anyw = pl.BlockSpec(memory_space=pltpu.HBM)
    dma = pltpu.SemaphoreType.DMA
    sums, start = pl.pallas_call(
        functools.partial(kernel, dims),
        out_shape=(
            jax.ShapeDtypeStruct((bags, width), F32),
            jax.ShapeDtypeStruct((samples, units), F32),
        ),
        in_specs=[anyw] * 6,
        out_specs=(vmem, vmem),
        scratch_shapes=[
            pltpu.VMEM((samples, lanes), I32),
            pltpu.VMEM((nt, samples), I32),
            pltpu.VMEM((samples, width), F32),
            pltpu.VMEM((1, units), F32),
            pltpu.VMEM((nt * local_rows, width), F32),
            pltpu.VMEM(w_dense.shape, F32),
            pltpu.VMEM((CHIPS, 1, 4 * cap), I32),
            pltpu.VMEM((CHIPS, 1, 4 * cap), I32),
            pltpu.SMEM((CHIPS, 1, 4 * cap), I32),
            pltpu.SMEM((CHIPS, 1, 4 * cap), I32),
            pltpu.VMEM((CHIPS, cap, width), F32),
            pltpu.VMEM((SIDE, cap, width), F32),
            pltpu.VMEM((CHIPS, cap, width), F32),
            pltpu.VMEM((CHIPS, bags, width), F32),
            pltpu.VMEM((CHIPS, bags, width), F32),
            pltpu.VMEM((groups, bags, width), F32),
            pltpu.VMEM((groups, bags, width), F32),
            dma((5,)),
            dma,
            dma,
            dma,
            dma,
            dma,
            dma((SIDE,)),
            dma,
            dma((groups,)),
            dma,
            dma((3, TEAMS)),
            dma((3, TEAMS)),
            dma,
            dma,
        ],
        compiler_params=pltpu.CompilerParams(
            collective_id=0, has_side_effects=True, vmem_limit_bytes=40 * 1024 * 1024
        ),
    )(
        *(
            pltpu.with_memory_space_constraint(v, pltpu.HBM)
            for v in (
                bag_index,
                bag_length.T,
                emb_tables.reshape(nt * local_rows, width),
                dense_feats,
                w_dense,
                top_bias.reshape(1, units),
            )
        )
    )
    return pl.pallas_call(
        interact,
        out_shape=(
            jax.ShapeDtypeStruct((samples, nt, width), F32),
            jax.ShapeDtypeStruct((samples, units), F32),
        ),
        in_specs=[vmem] * 4,
        out_specs=(vmem, vmem),
        compiler_params=pltpu.CompilerParams(vmem_limit_bytes=8 * 1024 * 1024),
    )(sums, start, dense_feats, w_pair)


def solution(mesh):
    in_specs = (
        P(("rows", "cols"), None),
        P(("rows", "cols"), None),
        P(None, ("rows", "cols"), None),
        P(("rows", "cols"), None),
        P(),
        P(),
        P(),
    )
    out_specs = (P(("rows", "cols"), None, None), P(("rows", "cols"), None))
    return jax.shard_map(
        shards, mesh=mesh, in_specs=in_specs, out_specs=out_specs, check_vma=False
    )
```
